32 devices in a mesh: sys: 4 (over x, core), slab: 8 (over z, y).
Axes of the slice: x: 2, y: 2, z: 4, core: 2. Of those that a mesh axis runs over, the one named last changes fastest.
Arguments:
- right_side: float32 [128, 512, 128], P('slab', 'sys'), parts along dimension 1, may hold values from -8 to 8
- diagonal: float32 [128, 512, 128], P('slab', 'sys'), parts along dimension 1, may hold values from 0.25 to 2
Outputs:
- solution_field: float32 [128, 512, 128], P('slab', 'sys'), parts along dimension 1
- residual: float32 [128, 512, 128], P('slab', 'sys'), parts along dimension 1
The draws below stay inside these ranges and needn't reach their ends.
There are 4 independent parts, one for each index of `sys`. The reference program is written for one: setup_inputs(seed, part) draws one part's arguments, and reference() takes and returns one part's arrays. A program takes and returns all parts, laid end to end along the dimension named above; each array names one. Nothing has to cross between parts.
All inputs are finite; a program needn't handle non-finite values.
Results may differ from the reference program's by a relative error of at most 0.0003.
Values sent between devices are 32-bit elements; how exact they have to be, the bound alone decides.
No kernel may reach another device: no remote copies, remote signals or barrier semaphores. Data moves between devices by JAX's collectives and lax.ppermute only.
A program may use at most 64 MiB of HBM per device.

```python
import math
import jax
import jax.numpy as jnp

NY = 128
NX = 128
ITERS = 10
NZ = 128


def draw_right_side(key, part):
    depth_index = jnp.arange(NZ, dtype=jnp.float32)
    scales = 3.0 ** (depth_index / max(NZ - 1, 1))
    values = jax.random.normal(key, (NZ, NY, NX), jnp.float32)
    return jnp.clip(values * scales[:, None, None], -8.0, 8.0)


def levels(rng, dims, shards, smallest, largest):
    level = 1.0
    for dim, blocks in shards:
        steps = jax.random.uniform(jax.random.fold_in(jax.random.fold_in(rng, 6), dim), (blocks,), jnp.float32, smallest / len(shards), largest / len(shards))
        level = level * jnp.repeat(jnp.exp(steps), dims[dim] // blocks).reshape((-1,) + (1,) * (len(dims) - 1 - dim))
    return level


def setup_inputs(seed: int = 0, part: int = 0) -> dict:
    splits = jax.random.split(jax.random.key(seed), 3)
    own_keys = jax.random.split(jax.random.fold_in(splits[2], part), 3)
    right_side = draw_right_side(jax.random.fold_in(jax.random.fold_in(splits[2], part), 71), part)
    diagonal = jnp.clip(jnp.exp(math.log(2.0) - 2.0794415 * jax.random.uniform(own_keys[1], (NZ, NY, NX), jnp.float32) ** levels(own_keys[1], (NZ, NY, NX), ((0, 8),), -0.2, 0.2)), 0.25, 2.0)
    return {"right_side": right_side, "diagonal": diagonal}


def operate(values, diagonal):
    padded = jnp.pad(values, 1)
    beside = padded[2:, 1:-1, 1:-1] + padded[:-2, 1:-1, 1:-1]
    beside = beside + padded[1:-1, 2:, 1:-1] + padded[1:-1, :-2, 1:-1]
    beside = beside + padded[1:-1, 1:-1, 2:] + padded[1:-1, 1:-1, :-2]
    return (6.0 + diagonal) * values - beside


def reference(right_side, diagonal):
    solution_field = jnp.zeros_like(right_side)
    residual = right_side
    direction = right_side
    norm_now = jnp.sum(residual * residual)
    for iteration in range(ITERS):
        applied = operate(direction, diagonal)
        step_size = norm_now / jnp.sum(direction * applied)
        solution_field = solution_field + step_size * direction
        residual = residual - step_size * applied
        norm_next = jnp.sum(residual * residual)
        direction = residual + (norm_next / norm_now) * direction
        norm_now = norm_next
    return solution_field, residual
```

```python
import functools

import jax
import jax.numpy as jnp
from jax import lax
from jax.experimental import pallas as pl
from jax.experimental.pallas import tpu as pltpu
from jax.sharding import PartitionSpec as P

FIRST = 5
SECOND = 4
LOW, HIGH = 0.25, 14.0
CENTER = (LOW + HIGH) / 2
HALF = (HIGH - LOW) / 2
ROWS, LANES = 16, 128
F32 = jnp.float32


def edges(shape):
    row = lax.broadcasted_iota(jnp.int32, shape, 0)
    lane = lax.broadcasted_iota(jnp.int32, shape, 1)
    return row == 0, row == shape[0] - 1, lane == 0, lane == shape[1] - 1


def advance(cur, above, below, diag, prev=None):
    first_row, last_row, first_lane, last_lane = edges(cur.shape)
    ny, nx = cur.shape
    zero = jnp.zeros_like(cur)
    beside = above + below
    beside = beside + jnp.where(first_row, zero, pltpu.roll(cur, 1, 0))
    beside = beside + jnp.where(last_row, zero, pltpu.roll(cur, ny - 1, 0))
    beside = beside + jnp.where(first_lane, zero, pltpu.roll(cur, 1, 1))
    beside = beside + jnp.where(last_lane, zero, pltpu.roll(cur, nx - 1, 1))
    image = ((6.0 - CENTER) + diag) * cur - beside
    if prev is None:
        return image * (1.0 / HALF)
    return image * (2.0 / HALF) - prev


def interior(cur, prev, diag, one, two):
    planes = cur.shape[0]

    def inner(z, carry):
        old = None if prev is None else prev[z]
        one[z] = advance(cur[z], cur[z + 1], cur[z - 1], diag[z], old)
        return carry

    def outer(z, carry):
        two[z] = advance(one[z], one[z + 1], one[z - 1], diag[z], cur[z])
        return carry

    lax.fori_loop(1, planes - 1, inner, 0)
    lax.fori_loop(2, planes - 2, outer, 0)


def boundary(where, got_a, got_b, cur, prev, ghost, diag, ghost_diag, one, two):
    last = cur.shape[0] - 1
    even = where[0] == 0
    has_low = where[1].astype(F32)
    has_high = where[2].astype(F32)
    pick = lambda k: (
        jnp.where(even, got_b[k], got_a[k]),
        jnp.where(even, got_a[k], got_b[k]),
    )
    (low_far, high_near), (low_near, high_far) = pick(0), pick(1)
    old = lambda ref, k: None if ref is None else ref[k]
    low = has_low * advance(low_near, cur[0], low_far, ghost_diag[0], old(ghost, 0))
    high = has_high * advance(high_near, high_far, cur[last], ghost_diag[1], old(ghost, 1))
    bottom = advance(cur[0], cur[1], low_near, diag[0], old(prev, 0))
    top = advance(cur[last], high_near, cur[last - 1], diag[last], old(prev, last))
    one[0] = bottom
    one[last] = top
    two[0] = advance(bottom, one[1], low, diag[0], cur[0])
    two[1] = advance(one[1], one[2], bottom, diag[1], cur[1])
    two[last] = advance(top, high, one[last - 1], diag[last], cur[last])
    two[last - 1] = advance(one[last - 1], top, one[last - 2], diag[last - 1], cur[last - 1])
    return low, high


def put_sides(where, field, side_a, side_b):
    even = where[0] == 0
    last = field.shape[0] - 1
    for k in range(2):
        low, high = field[k], field[last - 1 + k]
        side_a[k] = jnp.where(even, high, low)
        side_b[k] = jnp.where(even, low, high)


def grid_index():
    shape = (ROWS, LANES)
    return (
        lax.broadcasted_iota(jnp.int32, shape, 0),
        lax.broadcasted_iota(jnp.int32, shape, 1),
    )


def total(tile):
    return jnp.sum(jnp.sum(tile, axis=0, keepdims=True), axis=1, keepdims=True)


def unit(k):
    row = lax.broadcasted_iota(jnp.int32, (1, LANES), 1)
    col = lax.broadcasted_iota(jnp.int32, (ROWS, 1), 0)
    return (col == k).astype(F32), (row == k).astype(F32)


def axpy(scale, a, b):
    return a[0] + scale * b[0], a[1] + scale * b[1]


def apply(mat, mat_t, v):
    return (
        jnp.sum(mat * v[1], axis=1, keepdims=True),
        jnp.sum(mat_t * v[0], axis=0, keepdims=True),
    )


def form(gram, a, b):
    return total(a[0] * gram * b[1])


def steps(gram, mat, mat_t, x, r, p, count):
    norm = form(gram, r, r)
    for k in range(count):
        image = apply(mat, mat_t, p)
        size = norm / form(gram, p, image)
        x = axpy(size, x, p)
        r = axpy(-size, r, image)
        if k + 1 < count:
            new = form(gram, r, r)
            p = axpy(new / norm, r, p)
            norm = new
    return x, r, p, norm


def chebyshev_columns(first, count):
    ri, ci = grid_index()

    def one(ri, ci):
        inside = (ci >= first) & (ci < first + count)
        diag = jnp.where(inside & (ri == ci), CENTER, 0.0)
        down = jnp.where(ci == first, HALF, HALF / 2)
        diag = diag + jnp.where(inside & (ri == ci + 1), down, 0.0)
        return diag + jnp.where(inside & (ci > first) & (ri == ci - 1), HALF / 2, 0.0)

    return one(ri, ci), one(ci, ri)


def to_powers(size, count):
    ri, ci = grid_index()

    def one(ri, ci):
        j = ci - 1
        inside = (j >= 0) & (j < count)
        out = jnp.where((ci == 0) & (ri == 0), 1.0, 0.0)
        out = out + jnp.where(inside & (ri == j), 1.0 - size * CENTER, 0.0)
        down = jnp.where(j == 0, HALF, HALF / 2)
        out = out - jnp.where(inside & (ri == j + 1), size * down, 0.0)
        return out - jnp.where(inside & (j > 0) & (ri == j - 1), size * (HALF / 2), 0.0)

    return one(ri, ci), one(ci, ri)


def gram_tile(sums):
    ri, ci = grid_index()
    out = jnp.zeros((ROWS, LANES), F32)
    rows = {key: jnp.sum(val, axis=0, keepdims=True) for key, val in sums.items()}
    blank = jnp.zeros((1, LANES), F32)
    for j in sorted({j for _, j in rows}):
        stack = jnp.concatenate([rows.get((i, j), blank) for i in range(ROWS)], axis=0)
        col = jnp.sum(stack, axis=1, keepdims=True)
        out = out + jnp.where(ci == j, col, 0.0)
        row = jnp.sum(jnp.where(ri == ci, col, 0.0), axis=0, keepdims=True)
        out = out + jnp.where((ri == j) & (ci < j), row, 0.0)
    return out


def gather_sums(planes, ny, load, pairs):
    keys = list(pairs)

    def body(z, accs):
        accs = list(accs)
        for y in range(ny // 8):
            tiles = load(z, y)
            for k, (i, j) in enumerate(keys):
                accs[k] = accs[k] + tiles[i] * tiles[j]
        return tuple(accs)

    init = tuple(jnp.zeros((8, LANES), F32) for _ in keys)
    accs = lax.fori_loop(0, planes, body, init)
    return dict(zip(keys, accs))


def first_size(sums):
    norm = jnp.sum(sums[0:1, :], axis=1, keepdims=True)
    cross = jnp.sum(sums[1:2, :], axis=1, keepdims=True)
    return norm, norm / (CENTER * norm + HALF * cross)


def tile(ref, z, y):
    return ref[z, pl.ds(8 * y, 8), :]


def shifted(powers, size, count):
    keep = 1.0 - size * CENTER
    move = size * (HALF / 2)
    out = [powers[0], keep * powers[0] - (2.0 * move) * powers[1]]
    for j in range(1, count):
        out.append(keep * powers[j] - move * (powers[j + 1] + powers[j - 1]))
    return out


def call(kernel, outs, aliases=None):
    def run(*args):
        in_specs = [
            pl.BlockSpec(memory_space=pltpu.SMEM if a.dtype == jnp.int32 else pltpu.VMEM)
            for a in args
        ]
        return pl.pallas_call(
            kernel,
            out_shape=[jax.ShapeDtypeStruct(s, F32) for s in outs],
            in_specs=in_specs,
            out_specs=[pl.BlockSpec(memory_space=pltpu.VMEM) for _ in outs],
            input_output_aliases=aliases or {},
            compiler_params=pltpu.CompilerParams(vmem_limit_bytes=40 << 20),
        )(*args)

    return run


def start_kernel(cur, diag, one, two):
    interior(cur, None, diag, one, two)


def next_kernel(cur, prev, diag, one, two):
    interior(cur, prev, diag, one, two)


def next_sums_kernel(cur, prev, diag, rhs, one, two, sums):
    interior(cur, prev, diag, one, two)
    planes, ny, _ = cur.shape
    got = gather_sums(
        planes,
        ny,
        lambda z, y: {0: tile(rhs, z, y), 1: tile(prev, z, y)},
        [(0, 0), (0, 1)],
    )
    rows = [jnp.sum(got[key], axis=0, keepdims=True) for key in ((0, 0), (0, 1))]
    sums[...] = jnp.concatenate(rows + [jnp.zeros((6, LANES), F32)], axis=0)


def open_edge_kernel(where, got_a, got_b, cur, diag, one_in, two_in, one, two, side_a, side_b, ghost, ghost_diag):
    even = where[0] == 0
    ghost_diag[0] = jnp.where(even, got_b[2], got_a[2])
    ghost_diag[1] = jnp.where(even, got_a[2], got_b[2])
    low, high = boundary(where, got_a, got_b, cur, None, None, diag, ghost_diag, one, two)
    ghost[0] = low
    ghost[1] = high
    put_sides(where, two, side_a, side_b)


def restart_edge_kernel(where, got_a, got_b, cur, diag, ghost_diag, one_in, two_in, one, two, side_a, side_b, ghost):
    low, high = boundary(where, got_a, got_b, cur, None, None, diag, ghost_diag, one, two)
    ghost[0] = low
    ghost[1] = high
    put_sides(where, two, side_a, side_b)


def edge_kernel(where, got_a, got_b, cur, prev, old_ghost, diag, ghost_diag, one_in, two_in, one, two, side_a, side_b, ghost):
    low, high = boundary(where, got_a, got_b, cur, prev, old_ghost, diag, ghost_diag, one, two)
    ghost[0] = low
    ghost[1] = high
    put_sides(where, two, side_a, side_b)


def middle_kernel(where, got_a, got_b, cur, prev, old_ghost, diag, ghost_diag, one_in, two_in, sums, t0, t1, t2, one, two, gram):
    boundary(where, got_a, got_b, cur, prev, old_ghost, diag, ghost_diag, one, two)
    planes, ny, _ = cur.shape
    _, size = first_size(sums)
    refs = [t0, t1, t2, prev, cur, one, two]

    def load(z, y):
        return shifted([tile(ref, z, y) for ref in refs], size, FIRST + 1)

    n = FIRST + 2
    pairs = [(i, j) for j in range(1, n) for i in range(j + 1)]
    gram[...] = gram_tile(gather_sums(planes, ny, load, pairs))


def restart_kernel(where, sums, gram, *refs):
    powers = refs[: FIRST + 2]
    field, side_a, side_b, state = refs[FIRST + 2 :]
    norm, size = first_size(sums)
    ri, ci = grid_index()
    top = FIRST + 1
    mat_g = gram[...] + jnp.where((ri == 0) & (ci == 0), norm, 0.0)
    mat, mat_t = chebyshev_columns(1, FIRST)
    open_col = lambda ri, ci: jnp.where(
        ci == 0, jnp.where(ri == 0, 1.0 / size, jnp.where(ri == 1, -1.0 / size, 0.0)), 0.0
    )
    mat = mat + open_col(ri, ci)
    mat_t = mat_t + open_col(ci, ri)
    e0, e1 = unit(0), unit(1)
    x = (size * e0[0], size * e0[1])
    r = e1
    p = axpy(form(mat_g, r, r) / norm, r, e0)
    x, r, p, norm = steps(mat_g, mat, mat_t, x, r, p, FIRST)
    new = form(mat_g, r, r)
    direction = axpy(0.0, (new / norm * p[0], new / norm * p[1]), p)
    change, change_t = to_powers(size, FIRST + 1)
    coef = apply(change, change_t, r)[1]
    scale = [coef[0:1, i : i + 1] for i in range(FIRST + 2)]
    planes, ny, _ = field.shape

    def body(z, carry):
        for y in range(ny // 8):
            acc = scale[0] * tile(powers[0], z, y)
            for i in range(1, FIRST + 2):
                acc = acc + scale[i] * tile(powers[i], z, y)
            field[z, pl.ds(8 * y, 8), :] = acc
        return carry

    lax.fori_loop(0, planes, body, 0)
    put_sides(where, field, side_a, side_b)
    lead = jnp.sum(r[1] * unit(top)[1], axis=1, keepdims=True)
    e_top = unit(top)
    inverse = 1.0 / lead
    swap = tuple(e * (inverse - 1.0) - inverse * (v - lead * e) for e, v in zip(e_top, r))

    def rebase(v):
        return axpy(jnp.sum(v[1] * e_top[1], axis=1, keepdims=True), v, swap)

    p = axpy(1.0, e_top, rebase(direction))
    x = rebase(x)
    mat = mat + swap[0] * jnp.sum(jnp.where(ri == top, mat, 0.0), axis=0, keepdims=True)
    mat_t = mat_t + swap[1] * jnp.sum(jnp.where(ci == top, mat_t, 0.0), axis=1, keepdims=True)
    more, more_t = chebyshev_columns(top, SECOND)
    full = lambda v: jnp.broadcast_to(v, (ROWS, LANES))
    state[0] = jnp.where((ri < top) & (ci < top), mat_g, 0.0)
    state[1] = mat + more
    state[2] = mat_t + more_t
    state[3] = full(p[0])
    state[4] = full(p[1])
    state[5] = full(x[0])
    state[6] = full(x[1])


def late_sums_kernel(cur, prev, diag, sums, v0, t0, t1, t2, t3, t4, t5, one, two, gram):
    interior(cur, prev, diag, one, two)
    planes, ny, _ = cur.shape
    _, size = first_size(sums)
    refs = [t0, t1, t2, t3, t4, t5]
    top = FIRST + 1

    def load(z, y):
        out = shifted([tile(ref, z, y) for ref in refs], size, FIRST)
        return out + [tile(ref, z, y) for ref in (v0, prev, cur)]

    pairs = [(i, j) for j in range(top, top + 3) for i in range(j + 1)]
    gram[...] = gram_tile(gather_sums(planes, ny, load, pairs))


def last_edge_kernel(where, got_a, got_b, cur, prev, old_ghost, diag, ghost_diag, one_in, two_in, sums, early, v0, t0, t1, t2, t3, t4, t5, one, two, gram):
    boundary(where, got_a, got_b, cur, prev, old_ghost, diag, ghost_diag, one, two)
    planes, ny, _ = cur.shape
    _, size = first_size(sums)
    refs = [t0, t1, t2, t3, t4, t5]
    top = FIRST + 1

    def load(z, y):
        out = shifted([tile(ref, z, y) for ref in refs], size, FIRST)
        return out + [tile(ref, z, y) for ref in (v0, prev, cur, one, two)]

    pairs = [(i, j) for j in range(top + 3, top + 5) for i in range(j + 1)]
    gram[...] = early[...] + gram_tile(gather_sums(planes, ny, load, pairs))


def finish_kernel(sums, state, gram, t0, t1, t2, t3, t4, t5, v0, v1, v2, v3, v4, solution_field, residual):
    _, size = first_size(sums)
    ri, ci = grid_index()
    top = FIRST + 1
    mat_g = state[0] + gram[...]
    p = (state[3][:, 0:1], state[4][0:1, :])
    x = (state[5][:, 0:1], state[6][0:1, :])
    x, r, _, _ = steps(mat_g, state[1], state[2], x, unit(top), p, SECOND)
    change, change_t = to_powers(size, FIRST)
    keep = jnp.where((ri == ci) & (ri >= top), 1.0, 0.0)
    low = jnp.where(ri < top, 1.0, 0.0) * jnp.where(ci < top, 1.0, 0.0)
    change = change * low + keep
    change_t = change_t * low + keep
    cx = apply(change, change_t, x)[1]
    cr = apply(change, change_t, r)[1]
    refs = [t0, t1, t2, t3, t4, t5, v0, v1, v2, v3, v4]
    sx = [cx[0:1, i : i + 1] for i in range(len(refs))]
    sr = [cr[0:1, i : i + 1] for i in range(len(refs))]
    planes, ny, _ = t0.shape

    def body(z, carry):
        for y in range(ny // 8):
            tiles = [tile(ref, z, y) for ref in refs]
            ax, ar = sx[0] * tiles[0], sr[0] * tiles[0]
            for i in range(1, len(refs)):
                ar = ar + sr[i] * tiles[i]
                if i + 1 < len(refs):
                    ax = ax + sx[i] * tiles[i]
            solution_field[z, pl.ds(8 * y, 8), :] = ax
            residual[z, pl.ds(8 * y, 8), :] = ar
        return carry

    lax.fori_loop(0, planes, body, 0)


def pairings(count):
    first = [(i, i ^ 1) for i in range(count) if i ^ 1 < count]
    second = [(i, i + 1) for i in range(1, count - 1, 2)]
    return first, second + [(j, i) for i, j in second]


def exchange(side_a, side_b):
    first, second = pairings(lax.axis_size("slab"))
    return lax.ppermute(side_a, "slab", first), lax.ppermute(side_b, "slab", second)


def everywhere(value):
    count = lax.axis_size("slab")
    if count & (count - 1):
        return lax.psum(value, "slab")
    bit = 1
    while bit < count:
        masks = [bit] if 2 * bit >= count else [bit, 2 * bit, 3 * bit]
        others = [lax.ppermute(value, "slab", [(i, i ^ m) for i in range(count)]) for m in masks]
        for other in others:
            value = value + other
        bit *= 4
    return value


def local(right_side, diagonal):
    index = lax.axis_index("slab")
    count = lax.axis_size("slab")
    even = index % 2 == 0
    where = jnp.stack([index % 2, index > 0, index < count - 1]).astype(jnp.int32)
    field = right_side.shape
    two_planes = (2,) + field[1:]
    pair = [field, field]
    sides = [two_planes, two_planes]
    small = (ROWS, LANES)
    low = jnp.concatenate([right_side[:2], diagonal[:1]])
    high = jnp.concatenate([right_side[-2:], diagonal[-1:]])
    got = exchange(jnp.where(even, high, low), jnp.where(even, low, high))

    t0, d = right_side, diagonal
    t1, t2 = call(start_kernel, pair)(t0, d)
    t1, t2, sa, sb, ghost, gd = call(open_edge_kernel, pair + sides + [two_planes] * 2, {5: 0, 6: 1})(
        where, *got, t0, d, t1, t2
    )
    got = exchange(sa, sb)
    t3, t4, sums = call(next_sums_kernel, pair + [(8, LANES)])(t2, t1, d, t0)
    sums = everywhere(sums)
    t3, t4, sa, sb, ghost = call(edge_kernel, pair + sides + [two_planes], {8: 0, 9: 1})(
        where, *got, t2, t1, ghost, d, gd, t3, t4
    )
    got = exchange(sa, sb)
    t5, t6 = call(next_kernel, pair)(t4, t3, d)
    t5, t6, gram = call(middle_kernel, pair + [small], {8: 0, 9: 1})(
        where, *got, t4, t3, ghost, d, gd, t5, t6, sums, t0, t1, t2
    )
    gram = everywhere(gram)
    v0, sa, sb, state = call(restart_kernel, [field] + sides + [(7,) + small])(
        where, sums, gram, t0, t1, t2, t3, t4, t5, t6
    )
    got = exchange(sa, sb)
    v1, v2 = call(start_kernel, pair)(v0, d)
    v1, v2, sa, sb, ghost = call(restart_edge_kernel, pair + sides + [two_planes], {6: 0, 7: 1})(
        where, *got, v0, d, gd, v1, v2
    )
    got = exchange(sa, sb)
    v3, v4, early = call(late_sums_kernel, pair + [small])(v2, v1, d, sums, v0, t0, t1, t2, t3, t4, t5)
    v3, v4, gram = call(last_edge_kernel, pair + [small], {8: 0, 9: 1})(
        where, *got, v2, v1, ghost, d, gd, v3, v4, sums, early, v0, t0, t1, t2, t3, t4, t5
    )
    gram = everywhere(gram)
    return tuple(
        call(finish_kernel, pair)(sums, state, gram, t0, t1, t2, t3, t4, t5, v0, v1, v2, v3, v4)
    )


def solution(mesh):
    placed = (P("slab", "sys", None), P("slab", "sys", None))
    return jax.shard_map(
        local,
        mesh=mesh,
        in_specs=placed,
        out_specs=placed,
        check_vma=False,
    )
```

```python
import functools

import jax
import jax.numpy as jnp
from jax import lax
from jax.experimental import pallas as pl
from jax.experimental.pallas import tpu as pltpu
from jax.sharding import PartitionSpec as P

FIRST = 5
SECOND = 4
LOW, HIGH = 0.25, 14.0
CENTER = (LOW + HIGH) / 2
HALF = (HIGH - LOW) / 2
ROWS, LANES = 16, 128
F32 = jnp.float32


def tile(at, row):
    ref, z = at
    return ref[z, pl.ds(row, 8), :]


def advance(out, cur, above, below, scale, prev=None, keep=None):
    _, ny, nx = cur[0].shape
    row = lax.broadcasted_iota(jnp.int32, (8, nx), 0)
    lane = lax.broadcasted_iota(jnp.int32, (8, nx), 1)
    zero = jnp.zeros((8, nx), F32)
    for at in range(0, ny, 8):
        mid = tile(cur, at)
        beside = tile(above, at) + tile(below, at)
        if at:
            beside = beside + tile(cur, at - 1)
        else:
            beside = beside + jnp.where(row == 0, zero, pltpu.roll(mid, 1, 0))
        if at + 8 < ny:
            beside = beside + tile(cur, at + 1)
        else:
            beside = beside + jnp.where(row == 7, zero, pltpu.roll(mid, 7, 0))
        left = jnp.where(lane == 0, zero, pltpu.roll(mid, 1, 1))
        right = jnp.where(lane == nx - 1, zero, pltpu.roll(mid, nx - 1, 1))
        beside = beside + (left + right)
        image = tile(scale, at) * mid - (2.0 / HALF) * beside
        image = 0.5 * image if prev is None else image - tile(prev, at)
        if keep is not None:
            image = image * keep
        out[0][out[1], pl.ds(at, 8), :] = image


def scaled(diag):
    return (2.0 / HALF) * diag + (2.0 / HALF) * (6.0 - CENTER)


def over(first, last, most, body):
    count = last - first
    step = max(k for k in range(1, most + 1) if count % k == 0)

    def run(i, carry):
        for k in range(step):
            body(first + i * step + k)
        return carry

    lax.fori_loop(0, count // step, run, 0)


def interior(cur, prev, scale, one, two):
    planes = cur.shape[0]

    def inner(z):
        old = None if prev is None else (prev, z)
        advance((one, z), (cur, z), (cur, z + 1), (cur, z - 1), (scale, z), old)

    def outer(z):
        advance((two, z), (one, z), (one, z + 1), (one, z - 1), (scale, z), (cur, z))

    over(1, planes - 1, 7, inner)
    over(2, planes - 2, 6, outer)


def boundary(where, got_a, got_b, cur, prev, old_ghost, scale, ghost_scale, one, two, ghost, near):
    last = cur.shape[0] - 1
    even = where[0] == 0
    has_low = where[1].astype(F32)
    has_high = where[2].astype(F32)
    for k in range(2):
        near[k] = jnp.where(even, got_b[k], got_a[k])
        near[2 + k] = jnp.where(even, got_a[k], got_b[k])
    old = lambda ref, k: None if ref is None else (ref, k)
    advance((ghost, 0), (near, 1), (cur, 0), (near, 0), (ghost_scale, 0), old(old_ghost, 0), has_low)
    advance((ghost, 1), (near, 2), (near, 3), (cur, last), (ghost_scale, 1), old(old_ghost, 1), has_high)
    advance((one, 0), (cur, 0), (cur, 1), (near, 1), (scale, 0), old(prev, 0))
    advance((one, last), (cur, last), (near, 2), (cur, last - 1), (scale, last), old(prev, last))
    advance((two, 0), (one, 0), (one, 1), (ghost, 0), (scale, 0), (cur, 0))
    advance((two, 1), (one, 1), (one, 2), (one, 0), (scale, 1), (cur, 1))
    advance((two, last), (one, last), (ghost, 1), (one, last - 1), (scale, last), (cur, last))
    top = last - 1
    advance((two, top), (one, top), (one, last), (one, top - 1), (scale, top), (cur, top))


def put_sides(where, field, side_a, side_b):
    even = where[0] == 0
    last = field.shape[0] - 1
    for k in range(2):
        low, high = field[k], field[last - 1 + k]
        side_a[k] = jnp.where(even, high, low)
        side_b[k] = jnp.where(even, low, high)


def row_index():
    return lax.broadcasted_iota(jnp.int32, (ROWS, LANES), 0)


def unit(k):
    return jnp.where(row_index() == k, 1.0, 0.0).astype(F32)


def entry(v, k):
    return jnp.broadcast_to(v[k : k + 1, :], (ROWS, LANES))


def columns(mat, count):
    return [jnp.broadcast_to(mat[:, j : j + 1], (ROWS, LANES)) for j in range(count)]


def product(cols, v):
    return functools.reduce(lambda a, b: a + b, [c * entry(v, k) for k, c in enumerate(cols)])


def dot(a, b):
    return jnp.broadcast_to(jnp.sum(a * b, axis=0, keepdims=True), (ROWS, LANES))


def steps(gram, mat, x, r, p, count):
    norm = dot(r, product(gram, r))
    for _ in range(count):
        image = product(mat, p)
        size = norm / dot(p, product(gram, image))
        x = x + size * p
        r = r - size * image
        new = dot(r, product(gram, r))
        last = (new / norm) * p
        p = r + last
        norm = new
    return x, r, last


def chebyshev_column(first, k):
    out = CENTER * unit(k) + (HALF if k == first else HALF / 2) * unit(k + 1)
    return out if k == first else out + (HALF / 2) * unit(k - 1)


def to_powers(size, count):
    cols = [unit(0)]
    for j in range(count):
        cols.append(unit(j) - size * chebyshev_column(0, j))
    return cols


def gram_tile(rows):
    ri = row_index()
    ci = lax.broadcasted_iota(jnp.int32, (ROWS, LANES), 1)
    out = jnp.zeros((ROWS, LANES), F32)
    blank = jnp.zeros((1, LANES), F32)
    for j in sorted({j for _, j in rows}):
        stack = jnp.concatenate([rows.get((i, j), blank) for i in range(ROWS)], axis=0)
        col = jnp.sum(stack, axis=1, keepdims=True)
        out = out + jnp.where(ci == j, col, 0.0)
        row = jnp.sum(jnp.where(ri == ci, col, 0.0), axis=0, keepdims=True)
        out = out + jnp.where((ri == j) & (ci < j), row, 0.0)
    return out


def inner_products(first, last, ny, load, pairs, acc):
    zero = jnp.zeros(acc.shape[1:], F32)
    for k in range(len(pairs)):
        acc[k] = zero

    def body(z, carry):
        sums = [None] * len(pairs)
        for row in range(0, ny, 8):
            tiles = load(z, row)
            for k, (i, j) in enumerate(pairs):
                part = tiles[i] * tiles[j]
                sums[k] = part if row == 0 else sums[k] + part
        for k, val in enumerate(sums):
            acc[k] = acc[k] + val
        return carry

    lax.fori_loop(first, last, body, 0)
    return {pair: jnp.sum(acc[k], axis=0, keepdims=True) for k, pair in enumerate(pairs)}


def pairs_of(first, last):
    return [(i, j) for j in range(first, last) for i in range(j + 1)]


def shifted(powers, size, count):
    keep = 1.0 - size * CENTER
    move = size * (HALF / 2)
    out = [powers[0], keep * powers[0] - (2.0 * move) * powers[1]]
    for j in range(1, count):
        out.append(keep * powers[j] - move * (powers[j + 1] + powers[j - 1]))
    return out


def first_size(sums):
    norm = jnp.sum(sums[0:1, :], axis=1, keepdims=True)
    cross = jnp.sum(sums[1:2, :], axis=1, keepdims=True)
    return norm / (CENTER * norm + HALF * cross)


def gathered(ref):
    return functools.reduce(lambda a, b: a + b, [ref[k] for k in range(ref.shape[0])])


def spread(ref, value):
    for k in range(ref.shape[0]):
        ref[k] = value


def call(kernel, outs, aliases=None, scratch=(), hbm=False):
    def spec(a):
        if a.dtype == jnp.int32:
            return pl.BlockSpec(memory_space=pltpu.SMEM)
        return pl.BlockSpec(memory_space=pltpu.HBM if hbm else pltpu.VMEM)

    def run(*args):
        return pl.pallas_call(
            kernel,
            out_shape=[jax.ShapeDtypeStruct(s, F32) for s in outs],
            in_specs=[spec(a) for a in args],
            out_specs=[pl.BlockSpec(memory_space=pltpu.VMEM) for _ in outs],
            scratch_shapes=list(scratch),
            input_output_aliases=aliases or {},
            compiler_params=pltpu.CompilerParams(vmem_limit_bytes=16 << 20),
        )(*args)

    return run


def side_kernel(where, rhs, diag, side_a, side_b, sems):
    even = where[0] == 0
    last = rhs.shape[0] - 1
    copies = []
    for k, (side, high) in enumerate(((side_a, even), (side_b, jnp.logical_not(even)))):
        field_at = jnp.where(high, last - 1, 0)
        diag_at = jnp.where(high, last, 0)
        copies.append(pltpu.make_async_copy(rhs.at[pl.ds(field_at, 2)], side.at[pl.ds(0, 2)], sems.at[2 * k]))
        copies.append(pltpu.make_async_copy(diag.at[pl.ds(diag_at, 1)], side.at[pl.ds(2, 1)], sems.at[2 * k + 1]))
    for copy in copies:
        copy.start()
    for copy in copies:
        copy.wait()


def open_kernel(rhs, diag, scale, one, two, sums, acc):
    planes, ny, _ = rhs.shape

    def fill(z):
        scale[z] = scaled(diag[z])

    over(0, planes, 4, fill)
    interior(rhs, None, scale, one, two)
    load = lambda z, row: [tile((rhs, z), row), tile((one, z), row)]
    rows = inner_products(1, planes - 1, ny, load, [(0, 0), (0, 1)], acc)
    blank = jnp.zeros((6, LANES), F32)
    spread(sums, jnp.concatenate([rows[0, 0], rows[0, 1], blank], axis=0))


def open_edge_kernel(where, got_a, got_b, cur, scale, sums, one_in, two_in, one, two, side_a, side_b, ghost, ghost_scale, size, near):
    even = where[0] == 0
    ghost_scale[0] = scaled(jnp.where(even, got_b[2], got_a[2]))
    ghost_scale[1] = scaled(jnp.where(even, got_a[2], got_b[2]))
    boundary(where, got_a, got_b, cur, None, None, scale, ghost_scale, one, two, ghost, near)
    put_sides(where, two, side_a, side_b)
    size[...] = jnp.broadcast_to(first_size(gathered(sums)), (8, LANES))


def restart_edge_kernel(where, got_a, got_b, cur, scale, ghost_scale, one_in, two_in, one, two, side_a, side_b, ghost, near):
    boundary(where, got_a, got_b, cur, None, None, scale, ghost_scale, one, two, ghost, near)
    put_sides(where, two, side_a, side_b)


def next_kernel(cur, prev, scale, one, two):
    interior(cur, prev, scale, one, two)


def edge_kernel(where, got_a, got_b, cur, prev, old_ghost, scale, ghost_scale, one_in, two_in, one, two, side_a, side_b, ghost, near):
    boundary(where, got_a, got_b, cur, prev, old_ghost, scale, ghost_scale, one, two, ghost, near)
    put_sides(where, two, side_a, side_b)


def partial_gram(field, vectors, size, count, extra, pairs, acc):
    planes, ny, _ = field.shape

    def load(z, row):
        powers = [tile((ref, z), row) for ref in vectors]
        return shifted(powers, size, count) + [tile((ref, z), row) for ref in extra]

    return gram_tile(inner_products(0, planes, ny, load, pairs, acc))


def third_kernel(cur, prev, scale, size, t0, t1, t2, one, two, gram, acc):
    interior(cur, prev, scale, one, two)
    gram[...] = partial_gram(cur, [t0, t1, t2, prev, cur], size[0:1, 0:1], FIRST - 1, [], pairs_of(0, FIRST), acc)


def third_edge_kernel(where, got_a, got_b, cur, prev, old_ghost, scale, ghost_scale, one_in, two_in, size, early, t0, t1, t2, one, two, gram, ghost, near, acc):
    boundary(where, got_a, got_b, cur, prev, old_ghost, scale, ghost_scale, one, two, ghost, near)
    late = partial_gram(
        cur, [t0, t1, t2, prev, cur, one, two], size[0:1, 0:1], FIRST + 1, [], pairs_of(FIRST, FIRST + 2), acc
    )
    spread(gram, early[...] + late)


def restart_kernel(where, size, gram, *refs):
    powers = refs[: FIRST + 2]
    field, side_a, side_b, state = refs[FIRST + 2 :]
    size = size[0:1, 0:1]
    top = FIRST + 1
    full = gathered(gram)
    mat = [(1.0 / size) * (unit(0) - unit(1))] + [chebyshev_column(1, k) for k in range(1, top)]
    zero = jnp.zeros((ROWS, LANES), F32)
    x, r, last = steps(columns(full, top + 1), mat, zero, unit(0), unit(0), top)
    coef = product(to_powers(size, top), r)
    scale = [coef[i : i + 1, :] for i in range(top + 1)]
    planes, ny, _ = field.shape

    def body(z, carry):
        for row in range(0, ny, 8):
            out = scale[0] * tile((powers[0], z), row)
            for i in range(1, top + 1):
                out = out + scale[i] * tile((powers[i], z), row)
            field[z, pl.ds(row, 8), :] = out
        return carry

    lax.fori_loop(0, planes, body, 0)
    put_sides(where, field, side_a, side_b)
    ri = row_index()
    ci = lax.broadcasted_iota(jnp.int32, (ROWS, LANES), 1)
    inverse = 1.0 / entry(r, top)
    swap = jnp.where(ri == top, inverse, -inverse * r)
    rebase = lambda v: jnp.where(ri == top, 0.0, v) + entry(v, top) * swap
    state[0] = jnp.where((ri < top) & (ci < top), full, 0.0)
    state[1] = unit(top) + rebase(last)
    state[2] = rebase(x)
    state[3] = swap


def fourth_kernel(cur, scale, size, t0, t1, t2, t3, t4, t5, one, two, gram, acc):
    interior(cur, None, scale, one, two)
    top = FIRST + 1
    gram[...] = partial_gram(
        cur, [t0, t1, t2, t3, t4, t5], size[0:1, 0:1], FIRST, [cur], pairs_of(top, top + 1), acc
    )


def fifth_kernel(cur, prev, scale, size, early, v0, t0, t1, t2, t3, t4, t5, one, two, gram, acc):
    interior(cur, prev, scale, one, two)
    top = FIRST + 1
    gram[...] = early[...] + partial_gram(
        cur, [t0, t1, t2, t3, t4, t5], size[0:1, 0:1], FIRST, [v0, prev, cur], pairs_of(top + 1, top + 3), acc
    )


def fifth_edge_kernel(where, got_a, got_b, cur, prev, old_ghost, scale, ghost_scale, one_in, two_in, size, early, v0, t0, t1, t2, t3, t4, t5, one, two, gram, ghost, near, acc):
    boundary(where, got_a, got_b, cur, prev, old_ghost, scale, ghost_scale, one, two, ghost, near)
    top = FIRST + 1
    late = partial_gram(
        cur, [t0, t1, t2, t3, t4, t5], size[0:1, 0:1], FIRST, [v0, prev, cur, one, two], pairs_of(top + 3, top + 5), acc
    )
    spread(gram, early[...] + late)


def finish_kernel(size, state, gram, *refs):
    top = FIRST + 1
    count = top + SECOND + 1
    refs, (solution_field, residual) = refs[:count], refs[count:]
    size = size[0:1, 0:1]
    mat = [(1.0 / size) * (unit(0) - unit(1))] + [chebyshev_column(1, k) for k in range(1, top - 1)]
    mat.append(CENTER * unit(top - 1) + (HALF / 2) * (unit(top - 2) + state[3]))
    mat += [chebyshev_column(top, k) for k in range(top, top + SECOND)]
    full = state[0] + gathered(gram)
    x, r, _ = steps(columns(full, count), mat, state[2], unit(top), state[1], SECOND)
    back = to_powers(size, FIRST) + [unit(k) for k in range(top, count)]
    x, r = product(back, x), product(back, r)
    sx = [x[i : i + 1, :] for i in range(count)]
    sr = [r[i : i + 1, :] for i in range(count)]
    planes, ny, _ = solution_field.shape

    def body(z, carry):
        for row in range(0, ny, 8):
            tiles = [tile((ref, z), row) for ref in refs]
            ax, ar = sx[0] * tiles[0], sr[0] * tiles[0]
            for i in range(1, count):
                ar = ar + sr[i] * tiles[i]
                if i + 1 < count:
                    ax = ax + sx[i] * tiles[i]
            solution_field[z, pl.ds(row, 8), :] = ax
            residual[z, pl.ds(row, 8), :] = ar
        return carry

    lax.fori_loop(0, planes, body, 0)


def pairings(count):
    first = [(i, i ^ 1) for i in range(count) if i ^ 1 < count]
    second = [(i, i + 1) for i in range(1, count - 1, 2)]
    return first, second + [(j, i) for i, j in second]


def exchange(side_a, side_b):
    first, second = pairings(lax.axis_size("slab"))
    return lax.ppermute(side_a, "slab", first), lax.ppermute(side_b, "slab", second)


def swap_all(value):
    return lax.all_to_all(value, "slab", 0, 0)


def local(right_side, diagonal):
    index = lax.axis_index("slab")
    count = lax.axis_size("slab")
    where = jnp.stack([index % 2, index > 0, index < count - 1]).astype(jnp.int32)
    field = right_side.shape
    some = lambda k: (k,) + field[1:]
    pair = [field, field]
    sides = [some(2), some(2)]
    small = (ROWS, LANES)
    wide = (count,) + small
    near = pltpu.VMEM(some(4), F32)
    ghost_near = (pltpu.VMEM(some(2), F32), near)
    acc = lambda k: pltpu.VMEM((k, 8, LANES), F32)

    sa, sb = call(side_kernel, [some(3)] * 2, scratch=(pltpu.SemaphoreType.DMA((4,)),), hbm=True)(
        where, right_side, diagonal
    )
    got = exchange(sa, sb)
    t0 = right_side
    d, t1, t2, sums = call(open_kernel, [field] + pair + [(count, 8, LANES)], scratch=(acc(2),))(t0, diagonal)
    sums = swap_all(sums)
    t1, t2, sa, sb, ghost, gd, size = call(
        open_edge_kernel, pair + sides + [some(2)] * 2 + [(8, LANES)], {6: 0, 7: 1}, (near,)
    )(where, *got, t0, d, sums, t1, t2)
    got = exchange(sa, sb)
    t3, t4 = call(next_kernel, pair)(t2, t1, d)
    t3, t4, sa, sb, ghost = call(edge_kernel, pair + sides + [some(2)], {8: 0, 9: 1}, (near,))(
        where, *got, t2, t1, ghost, d, gd, t3, t4
    )
    got = exchange(sa, sb)
    t5, t6, early = call(third_kernel, pair + [small], scratch=(acc(16),))(t4, t3, d, size, t0, t1, t2)
    t5, t6, gram = call(third_edge_kernel, pair + [wide], {8: 0, 9: 1}, ghost_near + (acc(16),))(
        where, *got, t4, t3, ghost, d, gd, t5, t6, size, early, t0, t1, t2
    )
    gram = swap_all(gram)
    v0, sa, sb, state = call(restart_kernel, [field] + sides + [(4,) + small])(
        where, size, gram, t0, t1, t2, t3, t4, t5, t6
    )
    got = exchange(sa, sb)
    powers = (t0, t1, t2, t3, t4, t5)
    v1, v2, early = call(fourth_kernel, pair + [small], scratch=(acc(8),))(v0, d, size, *powers)
    v1, v2, sa, sb, ghost = call(restart_edge_kernel, pair + sides + [some(2)], {6: 0, 7: 1}, (near,))(
        where, *got, v0, d, gd, v1, v2
    )
    got = exchange(sa, sb)
    v3, v4, early = call(fifth_kernel, pair + [small], scratch=(acc(24),))(v2, v1, d, size, early, v0, *powers)
    v3, v4, gram = call(fifth_edge_kernel, pair + [wide], {8: 0, 9: 1}, ghost_near + (acc(24),))(
        where, *got, v2, v1, ghost, d, gd, v3, v4, size, early, v0, *powers
    )
    gram = swap_all(gram)
    return tuple(call(finish_kernel, pair)(size, state, gram, *powers, v0, v1, v2, v3, v4))


def solution(mesh):
    placed = (P("slab", "sys", None), P("slab", "sys", None))
    return jax.shard_map(
        local,
        mesh=mesh,
        in_specs=placed,
        out_specs=placed,
        check_vma=False,
    )
```

```python
import functools

import jax
import jax.numpy as jnp
from jax import lax
from jax.experimental import pallas as pl
from jax.experimental.pallas import tpu as pltpu
from jax.sharding import PartitionSpec as P

FIRST = 4
SECOND = 5
WIDTH = 5
LOW, HIGH = 0.25, 14.0
CENTER = (LOW + HIGH) / 2
HALF = (HIGH - LOW) / 2
ROWS, LANES = 16, 128
F32 = jnp.float32


def tile(at, row):
    ref, z = at
    return ref[z, pl.ds(row, 8), :]


def advance(out, cur, above, below, scale, prev=None, keep=None):
    _, ny, nx = cur[0].shape
    row = lax.broadcasted_iota(jnp.int32, (8, nx), 0)
    lane = lax.broadcasted_iota(jnp.int32, (8, nx), 1)
    zero = jnp.zeros((8, nx), F32)
    for at in range(0, ny, 8):
        mid = tile(cur, at)
        beside = tile(above, at) + tile(below, at)
        if at:
            beside = beside + tile(cur, at - 1)
        else:
            beside = beside + jnp.where(row == 0, zero, pltpu.roll(mid, 1, 0))
        if at + 8 < ny:
            beside = beside + tile(cur, at + 1)
        else:
            beside = beside + jnp.where(row == 7, zero, pltpu.roll(mid, 7, 0))
        left = jnp.where(lane == 0, zero, pltpu.roll(mid, 1, 1))
        right = jnp.where(lane == nx - 1, zero, pltpu.roll(mid, nx - 1, 1))
        beside = beside + (left + right)
        image = tile(scale, at) * mid - (2.0 / HALF) * beside
        image = 0.5 * image if prev is None else image - tile(prev, at)
        if keep is not None:
            image = image * keep
        out[0][out[1], pl.ds(at, 8), :] = image


def scaled(diag):
    return (2.0 / HALF) * diag + (2.0 / HALF) * (6.0 - CENTER)


def over(first, last, most, body):
    count = last - first
    step = max(k for k in range(1, most + 1) if count % k == 0)

    def run(i, carry):
        for k in range(step):
            body(first + i * step + k)
        return carry

    lax.fori_loop(0, count // step, run, 0)


def interior(fields, scale):
    planes = scale.shape[0]
    for j in range(1, WIDTH + 1):

        def body(z, j=j):
            old = None if j == 1 else (fields[j - 2], z)
            cur = fields[j - 1]
            advance((fields[j], z), (cur, z), (cur, z + 1), (cur, z - 1), (scale, z), old)

        over(j, planes - j, 7, body)


def edge(where, use_a, planes):
    even = where[0] == 0
    high = even if use_a else jnp.logical_not(even)
    base = jnp.where(high, planes - 1, 0)
    inward = jnp.where(high, -1, 1)
    return high, base, inward, jnp.where(high, where[2], where[1]).astype(F32)


def wedge(fields, ghosts, scale, ghost_scale, base, inward, keep):
    def at(j, i):
        return (fields[j], base + inward * i) if i >= 0 else (ghosts[j], -1 - i)

    def scale_at(i):
        return (scale, base + inward * i) if i >= 0 else (ghost_scale, -1 - i)

    for j in range(1, WIDTH + 1):
        for i in range(j - WIDTH, j):
            old = None if j == 1 else at(j - 2, i)
            mask = keep if i < 0 else None
            advance(at(j, i), at(j - 1, i), at(j - 1, i + 1), at(j - 1, i - 1), scale_at(i), old, mask)


def put_sides(where, field, side_a, side_b):
    planes = field.shape[0]
    for side, use_a in ((side_a, True), (side_b, False)):
        _, base, inward, _ = edge(where, use_a, planes)
        for k in range(WIDTH):
            side[k] = field[base + inward * k]


def row_index():
    return lax.broadcasted_iota(jnp.int32, (ROWS, LANES), 0)


def unit(k):
    return jnp.where(row_index() == k, 1.0, 0.0).astype(F32)


def entry(v, k):
    return jnp.broadcast_to(v[k : k + 1, :], (ROWS, LANES))


def columns(mat, count):
    return [jnp.broadcast_to(mat[:, j : j + 1], (ROWS, LANES)) for j in range(count)]


def product(cols, v):
    return functools.reduce(lambda a, b: a + b, [c * entry(v, k) for k, c in enumerate(cols)])


def dot(a, b):
    return jnp.broadcast_to(jnp.sum(a * b, axis=0, keepdims=True), (ROWS, LANES))


def steps(gram, mat, x, r, p, count):
    norm = dot(r, product(gram, r))
    for _ in range(count):
        image = product(mat, p)
        size = norm / dot(p, product(gram, image))
        x = x + size * p
        r = r - size * image
        new = dot(r, product(gram, r))
        last = (new / norm) * p
        p = r + last
        norm = new
    return x, r, last


def chebyshev_column(first, k):
    out = CENTER * unit(k) + (HALF if k == first else HALF / 2) * unit(k + 1)
    return out if k == first else out + (HALF / 2) * unit(k - 1)


def to_powers(size, count):
    cols = [unit(0)]
    for j in range(count):
        cols.append(unit(j) - size * chebyshev_column(0, j))
    return cols


def gram_tile(rows):
    ri = row_index()
    ci = lax.broadcasted_iota(jnp.int32, (ROWS, LANES), 1)
    out = jnp.zeros((ROWS, LANES), F32)
    blank = jnp.zeros((1, LANES), F32)
    for j in sorted({j for _, j in rows}):
        stack = jnp.concatenate([rows.get((i, j), blank) for i in range(ROWS)], axis=0)
        col = jnp.sum(stack, axis=1, keepdims=True)
        out = out + jnp.where(ci == j, col, 0.0)
        row = jnp.sum(jnp.where(ri == ci, col, 0.0), axis=0, keepdims=True)
        out = out + jnp.where((ri == j) & (ci < j), row, 0.0)
    return out


def inner_products(first, count, ny, load, pairs, acc):
    zero = jnp.zeros(acc.shape[1:], F32)
    for k in range(len(pairs)):
        acc[k] = zero

    def body(k, carry):
        z = first + k
        sums = [None] * len(pairs)
        for row in range(0, ny, 8):
            tiles = load(z, row)
            for k, (i, j) in enumerate(pairs):
                part = tiles[i] * tiles[j]
                sums[k] = part if row == 0 else sums[k] + part
        for k, val in enumerate(sums):
            acc[k] = acc[k] + val
        return carry

    lax.fori_loop(0, count, body, 0)
    return {pair: jnp.sum(acc[k], axis=0, keepdims=True) for k, pair in enumerate(pairs)}


def pairs_of(first, last):
    return [(i, j) for j in range(first, last) for i in range(j + 1)]


def shifted(powers, size, count):
    keep = 1.0 - size * CENTER
    move = size * (HALF / 2)
    out = [powers[0], keep * powers[0] - (2.0 * move) * powers[1]]
    for j in range(1, count):
        out.append(keep * powers[j] - move * (powers[j + 1] + powers[j - 1]))
    return out


def first_size(sums):
    norm = jnp.sum(sums[0:1, :], axis=1, keepdims=True)
    cross = jnp.sum(sums[1:2, :], axis=1, keepdims=True)
    return norm / (CENTER * norm + HALF * cross)


def gathered(ref):
    return functools.reduce(lambda a, b: a + b, [ref[k] for k in range(ref.shape[0])])


def spread(ref, value):
    for k in range(ref.shape[0]):
        ref[k] = value


def call(kernel, outs, aliases=None, scratch=(), hbm=False):
    def spec(a):
        if a.dtype == jnp.int32:
            return pl.BlockSpec(memory_space=pltpu.SMEM)
        return pl.BlockSpec(memory_space=pltpu.HBM if hbm else pltpu.VMEM)

    def run(*args):
        return pl.pallas_call(
            kernel,
            out_shape=[jax.ShapeDtypeStruct(s, F32) for s in outs],
            in_specs=[spec(a) for a in args],
            out_specs=[pl.BlockSpec(memory_space=pltpu.VMEM) for _ in outs],
            scratch_shapes=list(scratch),
            input_output_aliases=aliases or {},
            compiler_params=pltpu.CompilerParams(vmem_limit_bytes=16 << 20),
        )(*args)

    return run


def side_kernel(where, rhs, diag, side_a, side_b, sems):
    copies = []
    for side, use_a in ((side_a, True), (side_b, False)):
        _, base, inward, _ = edge(where, use_a, rhs.shape[0])
        for k in range(2 * WIDTH - 1):
            source = rhs.at[pl.ds(base + inward * k, 1)] if k < WIDTH else diag.at[pl.ds(base + inward * (k - WIDTH), 1)]
            copies.append(pltpu.make_async_copy(source, side.at[pl.ds(k, 1)], sems.at[len(copies)]))
    for copy in copies:
        copy.start()
    for copy in copies:
        copy.wait()


def open_kernel(rhs, diag, side_in, scale, *refs):
    powers, (side, sums, acc) = (rhs,) + refs[:WIDTH], refs[WIDTH:]
    planes, ny, _ = rhs.shape

    def fill(z):
        scale[z] = scaled(diag[z])

    over(0, planes, 4, fill)
    interior(powers, scale)
    load = lambda z, row: [tile((rhs, z), row), tile((powers[1], z), row)]
    rows = inner_products(1, planes - 2, ny, load, [(0, 0), (0, 1)], acc)
    blank = jnp.zeros((6, LANES), F32)
    spread(sums, jnp.concatenate([rows[0, 0], rows[0, 1], blank], axis=0))


def low_gram(powers, size, first, count, acc):
    ny = powers[0].shape[1]
    load = lambda z, row: shifted([tile((ref, z), row) for ref in powers], size, FIRST + 1)
    return gram_tile(inner_products(first, count, ny, load, pairs_of(0, FIRST + 2), acc))


def high_gram(powers, fields, size, first, count, acc):
    ny = powers[0].shape[1]

    def load(z, row):
        out = shifted([tile((ref, z), row) for ref in powers], size, FIRST)
        return out + [tile((ref, z), row) for ref in fields]

    top = FIRST + 1
    return gram_tile(inner_products(first, count, ny, load, pairs_of(top, top + SECOND + 1), acc))


def lower(base, high):
    return jnp.where(high, base - (WIDTH - 1), base)


def first_wedge_kernel(where, got, scale, sums, t0, *refs):
    powers, (ghost_scale, size, gram) = (t0,) + refs[WIDTH : 2 * WIDTH], refs[2 * WIDTH : 2 * WIDTH + 3]
    ghosts, acc = refs[2 * WIDTH + 3 : -1], refs[-1]
    high, base, inward, keep = edge(where, True, t0.shape[0])
    for k in range(WIDTH - 1):
        ghost_scale[k] = scaled(got[WIDTH + k])
    wedge(powers, (got,) + ghosts, scale, ghost_scale, base, inward, keep)
    size[...] = jnp.broadcast_to(first_size(gathered(sums)), (8, LANES))
    first = jnp.where(high, WIDTH, 0)
    gram[...] = low_gram(powers, size[0:1, 0:1], first, t0.shape[0] - WIDTH, acc)


def second_wedge_kernel(where, got, scale, size, early, t0, *refs):
    powers, (ghost_scale, gram) = (t0,) + refs[WIDTH : 2 * WIDTH], refs[2 * WIDTH : 2 * WIDTH + 2]
    ghosts, acc = refs[2 * WIDTH + 2 : -1], refs[-1]
    high, base, inward, keep = edge(where, False, t0.shape[0])
    for k in range(WIDTH - 1):
        ghost_scale[k] = scaled(got[WIDTH + k])
    wedge(powers, (got,) + ghosts, scale, ghost_scale, base, inward, keep)
    spread(gram, early[...] + low_gram(powers, size[0:1, 0:1], lower(base, high), WIDTH, acc))


def third_open_kernel(v0, scale, size, side_in, *refs):
    powers, refs = refs[: FIRST + 1], refs[FIRST + 1 :]
    fields, (side, gram, acc) = (v0,) + refs[:WIDTH], refs[WIDTH:]
    interior(fields, scale)
    gram[...] = high_gram(powers, fields, size[0:1, 0:1], WIDTH, v0.shape[0] - 2 * WIDTH, acc)


def third_wedge(use_a, where, got, scale, ghost_scale, size, early, v0, *refs):
    powers, refs = refs[: FIRST + 1], refs[FIRST + 1 :]
    fields, gram = (v0,) + refs[WIDTH : 2 * WIDTH], refs[2 * WIDTH]
    ghosts, acc = refs[2 * WIDTH + 1 : -1], refs[-1]
    high, base, inward, keep = edge(where, use_a, v0.shape[0])
    wedge(fields, (got,) + ghosts, scale, ghost_scale, base, inward, keep)
    value = early[...] + high_gram(powers, fields, size[0:1, 0:1], lower(base, high), WIDTH, acc)
    if use_a:
        gram[...] = value
    else:
        spread(gram, value)


def restart_kernel(where, size, gram, *refs):
    powers = refs[: FIRST + 2]
    field, side_a, side_b, state = refs[FIRST + 2 :]
    size = size[0:1, 0:1]
    top = FIRST + 1
    full = gathered(gram)
    mat = [(1.0 / size) * (unit(0) - unit(1))] + [chebyshev_column(1, k) for k in range(1, top)]
    zero = jnp.zeros((ROWS, LANES), F32)
    x, r, last = steps(columns(full, top + 1), mat, zero, unit(0), unit(0), top)
    coef = product(to_powers(size, top), r)
    scale = [coef[i : i + 1, :] for i in range(top + 1)]
    planes, ny, _ = field.shape

    def body(z, carry):
        for row in range(0, ny, 8):
            out = scale[0] * tile((powers[0], z), row)
            for i in range(1, top + 1):
                out = out + scale[i] * tile((powers[i], z), row)
            field[z, pl.ds(row, 8), :] = out
        return carry

    lax.fori_loop(0, planes, body, 0)
    put_sides(where, field, side_a, side_b)
    ri = row_index()
    ci = lax.broadcasted_iota(jnp.int32, (ROWS, LANES), 1)
    inverse = 1.0 / entry(r, top)
    swap = jnp.where(ri == top, inverse, -inverse * r)
    rebase = lambda v: jnp.where(ri == top, 0.0, v) + entry(v, top) * swap
    state[0] = jnp.where((ri < top) & (ci < top), full, 0.0)
    state[1] = unit(top) + rebase(last)
    state[2] = rebase(x)
    state[3] = swap


def finish_kernel(size, state, gram, *refs):
    top = FIRST + 1
    count = top + SECOND + 1
    refs, (solution_field, residual) = refs[:count], refs[count:]
    size = size[0:1, 0:1]
    mat = [(1.0 / size) * (unit(0) - unit(1))] + [chebyshev_column(1, k) for k in range(1, top - 1)]
    mat.append(CENTER * unit(top - 1) + (HALF / 2) * (unit(top - 2) + state[3]))
    mat += [chebyshev_column(top, k) for k in range(top, top + SECOND)]
    full = state[0] + gathered(gram)
    x, r, _ = steps(columns(full, count), mat, state[2], unit(top), state[1], SECOND)
    back = to_powers(size, FIRST) + [unit(k) for k in range(top, count)]
    x, r = product(back, x), product(back, r)
    sx = [x[i : i + 1, :] for i in range(count)]
    sr = [r[i : i + 1, :] for i in range(count)]
    planes, ny, _ = solution_field.shape

    def body(z, carry):
        for row in range(0, ny, 8):
            tiles = [tile((ref, z), row) for ref in refs]
            ax, ar = sx[0] * tiles[0], sr[0] * tiles[0]
            for i in range(1, count):
                ar = ar + sr[i] * tiles[i]
                if i + 1 < count:
                    ax = ax + sx[i] * tiles[i]
            solution_field[z, pl.ds(row, 8), :] = ax
            residual[z, pl.ds(row, 8), :] = ar
        return carry

    lax.fori_loop(0, planes, body, 0)


def pairings(count):
    first = [(i, i ^ 1) for i in range(count) if i ^ 1 < count]
    second = [(i, i + 1) for i in range(1, count - 1, 2)]
    return first, second + [(j, i) for i, j in second]


def swap_a(side):
    return lax.ppermute(side, "slab", pairings(lax.axis_size("slab"))[0])


def swap_b(side):
    return lax.ppermute(side, "slab", pairings(lax.axis_size("slab"))[1])


def swap_all(value):
    return lax.all_to_all(value, "slab", 0, 0)


def local(right_side, diagonal):
    index = lax.axis_index("slab")
    count = lax.axis_size("slab")
    where = jnp.stack([index % 2, index > 0, index < count - 1]).astype(jnp.int32)
    field = right_side.shape
    some = lambda k: (k,) + field[1:]
    fields = [field] * WIDTH
    small = (ROWS, LANES)
    wide = (count,) + small
    ghosts = tuple(pltpu.VMEM(some(WIDTH - j), F32) for j in range(1, WIDTH))
    acc = lambda k: pltpu.VMEM((k, 8, LANES), F32)
    ghost_side = some(WIDTH - 1)

    message = some(2 * WIDTH - 1)
    sa, sb = call(
        side_kernel, [message] * 2, scratch=(pltpu.SemaphoreType.DMA((4 * WIDTH - 2,)),), hbm=True
    )(where, *(pltpu.with_memory_space_constraint(a, pltpu.HBM) for a in (right_side, diagonal)))
    got_a = swap_a(sa)
    t0 = right_side
    d, *powers, sb, sums = call(
        open_kernel, [field] + fields + [message, (count, 8, LANES)], {2: 1 + WIDTH}, (acc(2),)
    )(t0, diagonal, sb)
    got_b = swap_b(sb)
    sums = swap_all(sums)
    inner = {5 + k: k for k in range(WIDTH)}
    *powers, gd_a, size, early = call(
        first_wedge_kernel, fields + [ghost_side, (8, LANES), small], inner, ghosts + (acc(24),)
    )(where, got_a, d, sums, t0, *powers)
    inner = {6 + k: k for k in range(WIDTH)}
    *powers, gd_b, gram = call(second_wedge_kernel, fields + [ghost_side, wide], inner, ghosts + (acc(24),))(
        where, got_b, d, size, early, t0, *powers
    )
    gram = swap_all(gram)
    powers = [t0] + powers
    v0, sa, sb, state = call(restart_kernel, [field] + [some(WIDTH)] * 2 + [(4,) + small])(
        where, size, gram, *powers
    )
    powers = powers[: FIRST + 1]
    got_a = swap_a(sa)
    last = len(powers)
    *late, sb, early = call(third_open_kernel, fields + [some(WIDTH), small], {3: WIDTH}, (acc(56),))(
        v0, d, size, sb, *powers
    )
    got_b = swap_b(sb)
    inner = {7 + last + k: k for k in range(WIDTH)}
    *late, early = call(functools.partial(third_wedge, True), fields + [small], inner, ghosts + (acc(56),))(
        where, got_a, d, gd_a, size, early, v0, *powers, *late
    )
    *late, gram = call(functools.partial(third_wedge, False), fields + [wide], inner, ghosts + (acc(56),))(
        where, got_b, d, gd_b, size, early, v0, *powers, *late
    )
    gram = swap_all(gram)
    return tuple(call(finish_kernel, [field] * 2)(size, state, gram, *powers, v0, *late))


def solution(mesh):
    placed = (P("slab", "sys", None), P("slab", "sys", None))
    return jax.shard_map(
        local,
        mesh=mesh,
        in_specs=placed,
        out_specs=placed,
        check_vma=False,
    )
```

```python
import functools

import jax
import jax.numpy as jnp
from jax import lax
from jax.experimental import pallas as pl
from jax.experimental.pallas import tpu as pltpu
from jax.sharding import PartitionSpec as P

WIDTH = 5
LAST = 2 * WIDTH
LOW, HIGH = 0.25, 14.0
CENTER = (LOW + HIGH) / 2
HALF = (HIGH - LOW) / 2
ROWS, LANES = 16, 128
PARTS = 4
F32 = jnp.float32


def tile(at, row):
    ref, z = at
    return ref[z, pl.ds(row, 8), :]


def advance(out, cur, above, below, scale, prev=None, keep=None):
    _, ny, nx = cur[0].shape
    row = lax.broadcasted_iota(jnp.int32, (8, nx), 0)
    lane = lax.broadcasted_iota(jnp.int32, (8, nx), 1)
    zero = jnp.zeros((8, nx), F32)
    for at in range(0, ny, 8):
        mid = tile(cur, at)
        beside = tile(above, at) + tile(below, at)
        if at:
            beside = beside + tile(cur, at - 1)
        else:
            beside = beside + jnp.where(row == 0, zero, pltpu.roll(mid, 1, 0))
        if at + 8 < ny:
            beside = beside + tile(cur, at + 1)
        else:
            beside = beside + jnp.where(row == 7, zero, pltpu.roll(mid, 7, 0))
        left = jnp.where(lane == 0, zero, pltpu.roll(mid, 1, 1))
        right = jnp.where(lane == nx - 1, zero, pltpu.roll(mid, nx - 1, 1))
        beside = beside + (left + right)
        image = tile(scale, at) * mid - (2.0 / HALF) * beside
        image = 0.5 * image if prev is None else image - tile(prev, at)
        if keep is not None:
            image = image * keep
        out[0][out[1], pl.ds(at, 8), :] = image


def scaled(diag):
    return (2.0 / HALF) * diag + (2.0 / HALF) * (6.0 - CENTER)


def over(first, last, most, body):
    count = last - first
    step = max(k for k in range(1, most + 1) if count % k == 0)

    def run(i, carry):
        for k in range(step):
            body(first + i * step + k)
        return carry

    lax.fori_loop(0, count // step, run, 0)


def interior(fields, scale):
    planes = scale.shape[0]
    for j in range(1, WIDTH + 1):

        def body(z, j=j):
            old = None if j == 1 else (fields[j - 2], z)
            cur = fields[j - 1]
            advance((fields[j], z), (cur, z), (cur, z + 1), (cur, z - 1), (scale, z), old)

        over(j, planes - j, 7, body)


def edge(where, use_a, planes):
    even = where[0] == 0
    high = even if use_a else jnp.logical_not(even)
    base = jnp.where(high, planes - 1, 0)
    inward = jnp.where(high, -1, 1)
    return high, base, inward, jnp.where(high, where[2], where[1]).astype(F32)


def wedge(fields, got, ghosts, scale, ghost_scale, base, inward, keep):
    def at(j, i):
        if i >= 0:
            return fields[j], base + inward * i
        if j:
            return ghosts[j - 1], -1 - i
        return got, jnp.where(inward < 0, -1 - i, WIDTH + i)

    def scale_at(i):
        return (scale, base + inward * i) if i >= 0 else (ghost_scale, -1 - i)

    for j in range(1, WIDTH + 1):
        for i in range(j - WIDTH, j):
            old = None if j == 1 else at(j - 2, i)
            mask = keep if i < 0 else None
            advance(at(j, i), at(j - 1, i), at(j - 1, i + 1), at(j - 1, i - 1), scale_at(i), old, mask)


def lower(base, high, count=WIDTH):
    return jnp.where(high, base - (count - 1), base)


def put_sides(where, field, side_a, side_b):
    planes = field.shape[0]
    for side, use_a in ((side_a, True), (side_b, False)):
        high, base, _, _ = edge(where, use_a, planes)
        first = lower(base, high)
        for k in range(WIDTH):
            side[k] = field[first + k]


def row_index():
    return lax.broadcasted_iota(jnp.int32, (ROWS, LANES), 0)


def unit(k):
    return jnp.where(row_index() == k, 1.0, 0.0).astype(F32)


def entry(v, k):
    return jnp.broadcast_to(v[k : k + 1, :], (ROWS, LANES))


def columns(mat, count):
    return [jnp.broadcast_to(mat[:, j : j + 1], (ROWS, LANES)) for j in range(count)]


def product(cols, v):
    return functools.reduce(lambda a, b: a + b, [c * entry(v, k) for k, c in enumerate(cols)])


def dot(a, b):
    return jnp.broadcast_to(jnp.sum(a * b, axis=0, keepdims=True), (ROWS, LANES))


def steps(gram, mat, count):
    x, r, p = 0.0 * unit(0), unit(0), unit(0)
    norm = dot(r, product(gram, r))
    for _ in range(count):
        image = product(mat, p)
        size = norm / dot(p, product(gram, image))
        x = x + size * p
        r = r - size * image
        new = dot(r, product(gram, r))
        p = r + (new / norm) * p
        norm = new
    return x, r, norm


def chebyshev_column(first, k):
    out = CENTER * unit(k) + (HALF if k == first else HALF / 2) * unit(k + 1)
    return out if k == first else out + (HALF / 2) * unit(k - 1)


def to_powers(size, count):
    cols = [unit(0)]
    for j in range(count):
        cols.append(unit(j) - size * chebyshev_column(0, j))
    return cols


def gram_tile(rows):
    ri = row_index()
    ci = lax.broadcasted_iota(jnp.int32, (ROWS, LANES), 1)
    out = jnp.zeros((ROWS, LANES), F32)
    blank = jnp.zeros((1, LANES), F32)
    for j in sorted({j for _, j in rows}):
        stack = jnp.concatenate([rows.get((i, j), blank) for i in range(ROWS)], axis=0)
        col = jnp.sum(stack, axis=1, keepdims=True)
        out = out + jnp.where(ci == j, col, 0.0)
        row = jnp.sum(jnp.where(ri == ci, col, 0.0), axis=0, keepdims=True)
        out = out + jnp.where((ri == j) & (ci < j), row, 0.0)
    return out


def inner_products(first, count, ny, load, pairs, acc):
    zero = jnp.zeros(acc.shape[1:], F32)
    for k in range(len(pairs)):
        acc[k] = zero

    def body(k, carry):
        z = first + k
        sums = [None] * len(pairs)
        for row in range(0, ny, 8):
            tiles = load(z, row)
            for k, (i, j) in enumerate(pairs):
                part = tiles[i] * tiles[j]
                sums[k] = part if row == 0 else sums[k] + part
        for k, val in enumerate(sums):
            acc[k] = acc[k] + val
        return carry

    lax.fori_loop(0, count, body, 0)
    return {pair: jnp.sum(acc[k], axis=0, keepdims=True) for k, pair in enumerate(pairs)}


def pairs_of(first, last):
    return [(i, j) for j in range(first, last) for i in range(j + 1)]


def shifted(powers, size, count):
    keep = 1.0 - size * CENTER
    move = size * (HALF / 2)
    out = [powers[0], keep * powers[0] - (2.0 * move) * powers[1]]
    for j in range(1, count):
        out.append(keep * powers[j] - move * (powers[j + 1] + powers[j - 1]))
    return out


def gathered(ref):
    return functools.reduce(lambda a, b: a + b, [ref[k] for k in range(ref.shape[0])])


def spread(ref, value):
    for k in range(ref.shape[0]):
        ref[k] = value


def call(kernel, outs, aliases=None, scratch=(), hbm=(), out_space=pltpu.VMEM):
    def spec(k, a):
        if a.dtype == jnp.int32:
            return pl.BlockSpec(memory_space=pltpu.SMEM)
        return pl.BlockSpec(memory_space=pltpu.HBM if k in hbm else pltpu.VMEM)

    def run(*args):
        return pl.pallas_call(
            kernel,
            out_shape=[jax.ShapeDtypeStruct(s, F32) for s in outs],
            in_specs=[spec(k, a) for k, a in enumerate(args)],
            out_specs=[pl.BlockSpec(memory_space=out_space) for _ in outs],
            scratch_shapes=list(scratch),
            input_output_aliases=aliases or {},
            compiler_params=pltpu.CompilerParams(vmem_limit_bytes=16 << 20),
        )(*args)

    return run


def side_kernel(where, rhs, diag, side_a, side_b, sems):
    copies = []
    for side, use_a in ((side_a, True), (side_b, False)):
        high, base, _, _ = edge(where, use_a, rhs.shape[0])
        for source, at, count in ((rhs, 0, WIDTH), (diag, WIDTH, WIDTH - 1)):
            planes = source.at[pl.ds(lower(base, high, count), count)]
            copies.append(pltpu.make_async_copy(planes, side.at[pl.ds(at, count)], sems.at[len(copies)]))
    for copy in copies:
        copy.start()
    for copy in copies:
        copy.wait()


def open_kernel(rhs_far, diag_far, side_in, scale, *refs):
    powers, (side, gram, acc, diag, sems) = refs[: WIDTH + 1], refs[WIDTH + 1 :]
    rhs = powers[0]
    planes, ny, _ = rhs.shape
    copies = [
        pltpu.make_async_copy(far, near, sems.at[k])
        for k, (far, near) in enumerate(((diag_far, diag), (rhs_far, rhs)))
    ]
    for copy in copies:
        copy.start()
    for copy in copies:
        copy.wait()

    def fill(z):
        scale[z] = scaled(diag[z])

    over(0, planes, 4, fill)
    interior(powers, scale)
    load = lambda z, row: [tile((ref, z), row) for ref in powers]
    pairs = pairs_of(0, WIDTH + 1)
    spread(gram, gram_tile(inner_products(WIDTH, planes - 2 * WIDTH, ny, load, pairs, acc)))


def basis_gram(powers, fields, size, first, count, pairs, acc):
    ny = powers[0].shape[1]

    def load(z, row):
        out = shifted([tile((ref, z), row) for ref in powers], size, WIDTH - 1)
        return out + [tile((ref, z), row) for ref in fields]

    rows = {}
    for at in range(0, len(pairs), 26):
        rows.update(inner_products(first, count, ny, load, pairs[at : at + 26], acc))
    return gram_tile(rows)


def restart(sampled):
    gram = columns(sampled, WIDTH + 1)
    norm, cross = entry(gram[0], 0), entry(gram[0], 1)
    size = norm / (CENTER * norm + HALF * cross)
    size = jnp.where((size > 0.5 / HIGH) & (size < 2.0 / LOW), size, 1.0 / CENTER)
    _, coef, left = steps(gram, [chebyshev_column(0, k) for k in range(WIDTH)], WIDTH)
    plain = unit(WIDTH - 1) - size * chebyshev_column(0, WIDTH - 1)
    return size, jnp.where((left > 0.0) & (left < 0.25 * norm), coef, plain)


def wedges_kernel(where, got_a, got_b, scale, sampled, t0, *refs):
    powers, refs = (t0,) + refs[WIDTH : 2 * WIDTH], refs[2 * WIDTH :]
    ghost_scales, (field, side_a, side_b, state), refs = refs[:2], refs[2:6], refs[6:]
    ghosts = refs[: WIDTH - 1], refs[WIDTH - 1 :]
    planes, ny, _ = t0.shape
    for use_a, got, ghost_scale, ghost in zip((True, False), (got_a, got_b), ghost_scales, ghosts):
        high, base, inward, keep = edge(where, use_a, planes)
        for k in range(WIDTH - 1):
            ghost_scale[k] = scaled(got[jnp.where(high, WIDTH + k, 2 * WIDTH - 2 - k)])
        wedge(powers, got, ghost, scale, ghost_scale, base, inward, keep)
    size, coef = restart(gathered(sampled))
    state[0] = size
    state[1] = coef
    weights = [coef[i : i + 1, :] for i in range(WIDTH + 1)]

    def body(z, carry):
        for row in range(0, ny, 8):
            out = weights[0] * tile((powers[0], z), row)
            for i in range(1, WIDTH + 1):
                out = out + weights[i] * tile((powers[i], z), row)
            field[z, pl.ds(row, 8), :] = out
        return carry

    lax.fori_loop(0, planes, body, 0)
    put_sides(where, field, side_a, side_b)


LOW_PAIRS = pairs_of(0, WIDTH)
HIGH_PAIRS = pairs_of(WIDTH, LAST + 1)


def fresh_kernel(v0, scale, state, side_in, *refs):
    powers, refs = refs[:WIDTH], refs[WIDTH:]
    fields, (side, gram, acc) = (v0,) + refs[:WIDTH], refs[WIDTH:]
    planes = v0.shape[0]
    size = state[0, 0:1, 0:1]
    interior(fields, scale)
    gram[...] = basis_gram(powers, (), size, 0, planes, LOW_PAIRS, acc)


def inner_kernel(v0, state, early, *refs):
    powers, fields, (gram, acc) = refs[:WIDTH], (v0,) + refs[WIDTH : 2 * WIDTH], refs[2 * WIDTH :]
    inner = v0.shape[0] - 2 * WIDTH
    gram[...] = early[...] + basis_gram(powers, fields, state[0, 0:1, 0:1], WIDTH, inner, HIGH_PAIRS, acc)


def fresh_wedge(use_a, where, got, scale, ghost_scale, state, early, v0, *refs):
    powers, refs = refs[:WIDTH], refs[WIDTH:]
    fields, gram = (v0,) + refs[WIDTH : 2 * WIDTH], refs[2 * WIDTH]
    ghosts, acc = refs[2 * WIDTH + 1 : -1], refs[-1]
    high, base, inward, keep = edge(where, use_a, v0.shape[0])
    wedge(fields, got, ghosts, scale, ghost_scale, base, inward, keep)
    first = lower(base, high)
    late = basis_gram(powers, fields, state[0, 0:1, 0:1], first, WIDTH, HIGH_PAIRS, acc)
    if use_a:
        gram[...] = early[...] + late
    else:
        spread(gram, early[...] + late)


def operator_columns(size, coef):
    powers = [unit(0)]
    for j in range(WIDTH - 1):
        image = (1.0 / size) * (powers[j] - unit(1 + j)) - CENTER * powers[j]
        powers.append((1.0 / HALF) * image if j == 0 else (2.0 / HALF) * image - powers[j - 1])
    rest = unit(WIDTH) - product(powers, coef)
    powers.append(rest / entry(coef, WIDTH))
    beyond = (HALF / 2) * (powers[WIDTH] + powers[WIDTH - 2]) + CENTER * powers[WIDTH - 1]
    beyond = powers[WIDTH - 1] - size * beyond
    out = [(1.0 / size) * (unit(0) - unit(1))]
    out += [chebyshev_column(1, k) for k in range(1, WIDTH - 1)]
    out.append(CENTER * unit(WIDTH - 1) + (HALF / 2) * (unit(WIDTH - 2) + beyond))
    return out + [chebyshev_column(WIDTH, k) for k in range(WIDTH, LAST)]


def finish_kernel(state, gram, *refs):
    count = LAST + 1
    refs, outs, rooms, sems = refs[:count], refs[count : count + 2], refs[count + 2 : count + 4], refs[-1]
    size = state[0]
    full = columns(gathered(gram), count)
    x, r, _ = steps(full, operator_columns(size, state[1]), LAST)
    back = to_powers(size, WIDTH - 1) + [unit(k) for k in range(WIDTH, count)]
    x, r = product(back, x), product(back, r)
    sx = [x[i : i + 1, :] for i in range(count)]
    sr = [r[i : i + 1, :] for i in range(count)]
    planes, ny, _ = refs[0].shape

    def body(z, carry):
        for row in range(0, ny, 8):
            tiles = [tile((ref, z), row) for ref in refs]
            ax, ar = sx[0] * tiles[0], sr[0] * tiles[0]
            for i in range(1, count):
                ar = ar + sr[i] * tiles[i]
                if i + 1 < count:
                    ax = ax + sx[i] * tiles[i]
            rooms[0][z, pl.ds(row, 8), :] = ax
            rooms[1][z, pl.ds(row, 8), :] = ar
        return carry

    copies = []
    part = planes // PARTS
    for k in range(PARTS):
        lax.fori_loop(k * part, (k + 1) * part, body, 0)
        here = pl.ds(k * part, part)
        for room, out in zip(rooms, outs):
            copies.append(pltpu.make_async_copy(room.at[here], out.at[here], sems.at[len(copies)]))
            copies[-1].start()
    for copy in copies:
        copy.wait()


def pairings(count):
    first = [(i, i ^ 1) for i in range(count) if i ^ 1 < count]
    second = [(i, i + 1) for i in range(1, count - 1, 2)]
    return first, second + [(j, i) for i, j in second]


def swap_a(side):
    return lax.ppermute(side, "slab", pairings(lax.axis_size("slab"))[0])


def swap_b(side):
    return lax.ppermute(side, "slab", pairings(lax.axis_size("slab"))[1])


def swap_all(value):
    return lax.all_to_all(value, "slab", 0, 0)


def local(right_side, diagonal):
    index = lax.axis_index("slab")
    count = lax.axis_size("slab")
    where = jnp.stack([index % 2, index > 0, index < count - 1]).astype(jnp.int32)
    field = right_side.shape
    some = lambda k: (k,) + field[1:]
    fields = [field] * WIDTH
    small = (ROWS, LANES)
    wide = (count,) + small
    ghosts = tuple(pltpu.VMEM(some(WIDTH - j), F32) for j in range(1, WIDTH))
    acc = lambda k: pltpu.VMEM((k, 8, LANES), F32)
    ghost_side = some(WIDTH - 1)

    message = some(2 * WIDTH - 1)
    rhs, diag = (pltpu.with_memory_space_constraint(a, pltpu.HBM) for a in (right_side, diagonal))
    semaphores = pltpu.SemaphoreType.DMA
    sa, sb = call(side_kernel, [message] * 2, scratch=(semaphores((4,)),), hbm=(1, 2))(where, rhs, diag)
    got_a = swap_a(sa)
    d, t0, *powers, sb, sampled = call(
        open_kernel,
        [field] * 2 + fields + [message, wide],
        {2: 2 + WIDTH},
        (acc(24), pltpu.VMEM(field, F32), semaphores((2,))),
        hbm=(0, 1),
    )(rhs, diag, sb)
    got_b = swap_b(sb)
    sampled = swap_all(sampled)
    inner = {6 + k: k for k in range(WIDTH)}
    side = some(WIDTH)
    *powers, gd_a, gd_b, v0, sa, sb, state = call(
        wedges_kernel, fields + [ghost_side] * 2 + [field, side, side, (2,) + small], inner, ghosts * 2
    )(where, got_a, got_b, d, sampled, t0, *powers)
    powers = [t0] + powers[:-1]
    got_a = swap_a(sa)
    *late, sb, early = call(fresh_kernel, fields + [side, small], {3: WIDTH}, (acc(26),))(v0, d, state, sb, *powers)
    got_b = swap_b(sb)
    early = call(inner_kernel, [small], scratch=(acc(26),))(v0, state, early, *powers, *late)[0]
    inner = {7 + WIDTH + k: k for k in range(WIDTH)}
    scratch = ghosts + (acc(26),)
    *late, early = call(functools.partial(fresh_wedge, True), fields + [small], inner, scratch)(
        where, got_a, d, gd_a, state, early, v0, *powers, *late
    )
    *late, gram = call(functools.partial(fresh_wedge, False), fields + [wide], inner, scratch)(
        where, got_b, d, gd_b, state, early, v0, *powers, *late
    )
    gram = swap_all(gram)
    rooms = (pltpu.VMEM(field, F32),) * 2 + (semaphores((2 * PARTS,)),)
    finish = call(finish_kernel, [field] * 2, scratch=rooms, out_space=pltpu.HBM)
    return tuple(finish(state, gram, *powers, v0, *late))


def solution(mesh):
    placed = (P("slab", "sys", None), P("slab", "sys", None))
    return jax.shard_map(
        local,
        mesh=mesh,
        in_specs=placed,
        out_specs=placed,
        check_vma=False,
    )
```

```python
import functools

import jax
import jax.numpy as jnp
from jax import lax
from jax.experimental import pallas as pl
from jax.experimental.pallas import tpu as pltpu
from jax.sharding import PartitionSpec as P

WIDTH = 5
LAST = 2 * WIDTH
LOW, HIGH = 0.25, 14.0
CENTER = (LOW + HIGH) / 2
HALF = (HIGH - LOW) / 2
ROWS, LANES = 16, 128
PARTS = 8
F32 = jnp.float32


def tile(at, row):
    ref, z = at
    return ref[z, pl.ds(row, 8), :]


def advance(out, cur, above, below, scale, prev=None, keep=None):
    _, ny, nx = cur[0].shape
    row = lax.broadcasted_iota(jnp.int32, (8, nx), 0)
    lane = lax.broadcasted_iota(jnp.int32, (8, nx), 1)
    zero = jnp.zeros((8, nx), F32)
    for at in range(0, ny, 8):
        mid = tile(cur, at)
        beside = tile(above, at) + tile(below, at)
        if at:
            beside = beside + tile(cur, at - 1)
        else:
            beside = beside + jnp.where(row == 0, zero, pltpu.roll(mid, 1, 0))
        if at + 8 < ny:
            beside = beside + tile(cur, at + 1)
        else:
            beside = beside + jnp.where(row == 7, zero, pltpu.roll(mid, 7, 0))
        left = jnp.where(lane == 0, zero, pltpu.roll(mid, 1, 1))
        right = jnp.where(lane == nx - 1, zero, pltpu.roll(mid, nx - 1, 1))
        beside = beside + (left + right)
        image = tile(scale, at) * mid - (2.0 / HALF) * beside
        image = 0.5 * image if prev is None else image - tile(prev, at)
        if keep is not None:
            image = image * keep
        out[0][out[1], pl.ds(at, 8), :] = image


def scaled(diag):
    return (2.0 / HALF) * diag + (2.0 / HALF) * (6.0 - CENTER)


def over(first, last, most, body):
    count = last - first
    step = max(k for k in range(1, most + 1) if count % k == 0)

    def run(i, carry):
        for k in range(step):
            body(first + i * step + k)
        return carry

    lax.fori_loop(0, count // step, run, 0)


def interior(fields, scale):
    planes = scale.shape[0]
    for j in range(1, WIDTH + 1):

        def body(z, j=j):
            old = None if j == 1 else (fields[j - 2], z)
            cur = fields[j - 1]
            advance((fields[j], z), (cur, z), (cur, z + 1), (cur, z - 1), (scale, z), old)

        over(j, planes - j, 7, body)


def edge(where, use_a, planes):
    even = where[0] == 0
    high = even if use_a else jnp.logical_not(even)
    base = jnp.where(high, planes - 1, 0)
    inward = jnp.where(high, -1, 1)
    return high, base, inward, jnp.where(high, where[2], where[1]).astype(F32)


def wedge(fields, got, ghosts, scale, ghost_scale, base, inward, keep):
    def at(j, i):
        if i >= 0:
            return fields[j], base + inward * i
        if j:
            return ghosts[j - 1], -1 - i
        return got, jnp.where(inward < 0, -1 - i, WIDTH + i)

    def scale_at(i):
        return (scale, base + inward * i) if i >= 0 else (ghost_scale, -1 - i)

    for j in range(1, WIDTH + 1):
        for i in range(j - WIDTH, j):
            old = None if j == 1 else at(j - 2, i)
            mask = keep if i < 0 else None
            advance(at(j, i), at(j - 1, i), at(j - 1, i + 1), at(j - 1, i - 1), scale_at(i), old, mask)


def lower(base, high, count=WIDTH):
    return jnp.where(high, base - (count - 1), base)


def put_sides(where, field, side_a, side_b):
    planes = field.shape[0]
    for side, use_a in ((side_a, True), (side_b, False)):
        high, base, _, _ = edge(where, use_a, planes)
        first = lower(base, high)
        for k in range(WIDTH):
            side[k] = field[first + k]


def row_index():
    return lax.broadcasted_iota(jnp.int32, (ROWS, LANES), 0)


def unit(k):
    return jnp.where(row_index() == k, 1.0, 0.0).astype(F32)


def entry(v, k):
    return jnp.broadcast_to(v[k : k + 1, :], (ROWS, LANES))


def columns(mat, count):
    return [jnp.broadcast_to(mat[:, j : j + 1], (ROWS, LANES)) for j in range(count)]


def product(cols, v):
    return functools.reduce(lambda a, b: a + b, [c * entry(v, k) for k, c in enumerate(cols)])


def dot(a, b):
    return jnp.broadcast_to(jnp.sum(a * b, axis=0, keepdims=True), (ROWS, LANES))


def steps(gram, mat, count):
    x, r, p = 0.0 * unit(0), unit(0), unit(0)
    norm = dot(r, product(gram, r))
    for _ in range(count):
        image = product(mat, p)
        size = norm / dot(p, product(gram, image))
        x = x + size * p
        r = r - size * image
        new = dot(r, product(gram, r))
        p = r + (new / norm) * p
        norm = new
    return x, r, norm


def chebyshev_column(first, k):
    out = CENTER * unit(k) + (HALF if k == first else HALF / 2) * unit(k + 1)
    return out if k == first else out + (HALF / 2) * unit(k - 1)


def to_powers(size, count):
    cols = [unit(0)]
    for j in range(count):
        cols.append(unit(j) - size * chebyshev_column(0, j))
    return cols


def gram_tile(rows):
    ri = row_index()
    ci = lax.broadcasted_iota(jnp.int32, (ROWS, LANES), 1)
    out = jnp.zeros((ROWS, LANES), F32)
    blank = jnp.zeros((1, LANES), F32)
    for j in sorted({j for _, j in rows}):
        stack = jnp.concatenate([rows.get((i, j), blank) for i in range(ROWS)], axis=0)
        col = jnp.sum(stack, axis=1, keepdims=True)
        out = out + jnp.where(ci == j, col, 0.0)
        row = jnp.sum(jnp.where(ri == ci, col, 0.0), axis=0, keepdims=True)
        out = out + jnp.where((ri == j) & (ci < j), row, 0.0)
    return out


def inner_products(ny, load, segments, acc):
    pairs = list(dict.fromkeys(pair for _, _, some in segments for pair in some))
    zero = jnp.zeros(acc.shape[1:], F32)
    for k in range(len(pairs)):
        acc[k] = zero
    for first, count, some in segments:
        for at in range(0, len(some), 30):

            def body(k, carry, first=first, some=some[at : at + 30]):
                sums = [None] * len(some)
                for row in range(0, ny, 8):
                    tiles = load(first + k, row)
                    for at, (i, j) in enumerate(some):
                        part = tiles[i] * tiles[j]
                        sums[at] = part if row == 0 else sums[at] + part
                for pair, val in zip(some, sums):
                    here = pairs.index(pair)
                    acc[here] = acc[here] + val
                return carry

            lax.fori_loop(0, count, body, 0)
    return {pair: jnp.sum(acc[k], axis=0, keepdims=True) for k, pair in enumerate(pairs)}


def pairs_of(first, last):
    return [(i, j) for j in range(first, last) for i in range(j + 1)]


def shifted(powers, size, count):
    keep = 1.0 - size * CENTER
    move = size * (HALF / 2)
    out = [powers[0], keep * powers[0] - (2.0 * move) * powers[1]]
    for j in range(1, count):
        out.append(keep * powers[j] - move * (powers[j + 1] + powers[j - 1]))
    return out


def gathered(ref):
    return functools.reduce(lambda a, b: a + b, [ref[k] for k in range(ref.shape[0])])


def spread(ref, value):
    for k in range(ref.shape[0]):
        ref[k] = value


def call(kernel, outs, aliases=None, scratch=(), hbm=(), out_space=pltpu.VMEM):
    def spec(k, a):
        if a.dtype == jnp.int32:
            return pl.BlockSpec(memory_space=pltpu.SMEM)
        return pl.BlockSpec(memory_space=pltpu.HBM if k in hbm else pltpu.VMEM)

    def run(*args):
        return pl.pallas_call(
            kernel,
            out_shape=[jax.ShapeDtypeStruct(s, F32) for s in outs],
            in_specs=[spec(k, a) for k, a in enumerate(args)],
            out_specs=[pl.BlockSpec(memory_space=out_space) for _ in outs],
            scratch_shapes=list(scratch),
            input_output_aliases=aliases or {},
            compiler_params=pltpu.CompilerParams(vmem_limit_bytes=16 << 20),
        )(*args)

    return run


def side_kernel(where, rhs, diag, side_a, side_b, sems):
    copies = []
    for side, use_a in ((side_a, True), (side_b, False)):
        high, base, _, _ = edge(where, use_a, rhs.shape[0])
        for source, at, count in ((rhs, 0, WIDTH), (diag, WIDTH, WIDTH - 1)):
            planes = source.at[pl.ds(lower(base, high, count), count)]
            copies.append(pltpu.make_async_copy(planes, side.at[pl.ds(at, count)], sems.at[len(copies)]))
    for copy in copies:
        copy.start()
    for copy in copies:
        copy.wait()


def open_kernel(rhs_far, diag_far, side_in, scale, *refs):
    powers, (side, gram, acc, diag, sems) = refs[: WIDTH + 1], refs[WIDTH + 1 :]
    rhs = powers[0]
    planes, ny, _ = rhs.shape
    copies = [
        pltpu.make_async_copy(far, near, sems.at[k])
        for k, (far, near) in enumerate(((diag_far, diag), (rhs_far, rhs)))
    ]
    for copy in copies:
        copy.start()
    for copy in copies:
        copy.wait()

    def fill(z):
        scale[z] = scaled(diag[z])

    over(0, planes, 4, fill)
    interior(powers, scale)
    load = lambda z, row: [tile((ref, z), row) for ref in powers]
    segments = [(WIDTH, planes - 2 * WIDTH, pairs_of(0, WIDTH + 1))]
    spread(gram, gram_tile(inner_products(ny, load, segments, acc)))


def basis_gram(powers, fields, size, segments, acc):
    ny = powers[0].shape[1]

    def load(z, row):
        out = shifted([tile((ref, z), row) for ref in powers], size, WIDTH - 1)
        return out + [tile((ref, z), row) for ref in fields]

    return gram_tile(inner_products(ny, load, segments, acc))


def restart(sampled):
    gram = columns(sampled, WIDTH + 1)
    norm, cross = entry(gram[0], 0), entry(gram[0], 1)
    size = norm / (CENTER * norm + HALF * cross)
    size = jnp.where((size > 0.5 / HIGH) & (size < 2.0 / LOW), size, 1.0 / CENTER)
    _, coef, left = steps(gram, [chebyshev_column(0, k) for k in range(WIDTH)], WIDTH)
    plain = unit(WIDTH - 1) - size * chebyshev_column(0, WIDTH - 1)
    return size, jnp.where((left > 0.0) & (left < 0.25 * norm), coef, plain)


def wedges_kernel(where, got_a, got_b, scale, sampled, t0, *refs):
    powers, refs = (t0,) + refs[WIDTH : 2 * WIDTH], refs[2 * WIDTH :]
    ghost_scales, (field, side_a, side_b, state), refs = refs[:2], refs[2:6], refs[6:]
    ghosts = refs[: WIDTH - 1], refs[WIDTH - 1 :]
    planes, ny, _ = t0.shape
    for use_a, got, ghost_scale, ghost in zip((True, False), (got_a, got_b), ghost_scales, ghosts):
        high, base, inward, keep = edge(where, use_a, planes)
        for k in range(WIDTH - 1):
            ghost_scale[k] = scaled(got[jnp.where(high, WIDTH + k, 2 * WIDTH - 2 - k)])
        wedge(powers, got, ghost, scale, ghost_scale, base, inward, keep)
    size, coef = restart(gathered(sampled))
    state[0] = size
    state[1] = coef
    weights = [coef[i : i + 1, :] for i in range(WIDTH + 1)]

    def body(z, carry):
        for row in range(0, ny, 8):
            out = weights[0] * tile((powers[0], z), row)
            for i in range(1, WIDTH + 1):
                out = out + weights[i] * tile((powers[i], z), row)
            field[z, pl.ds(row, 8), :] = out
        return carry

    lax.fori_loop(0, planes, body, 0)
    put_sides(where, field, side_a, side_b)


LOW_PAIRS = pairs_of(0, WIDTH)
CROSS_PAIRS = [(i, j) for i, j in pairs_of(WIDTH, LAST + 1) if i < WIDTH]
HIGH_PAIRS = CROSS_PAIRS + [pair for pair in pairs_of(WIDTH, LAST + 1) if pair[0] >= WIDTH]


def side_segments(base, inward, early):
    some = lambda i: [pair for pair in HIGH_PAIRS if (pair[1] - WIDTH <= i) == early]
    return [(base + inward * i, 1, some(i)) for i in range(WIDTH)]


def fresh_kernel(v0, scale, state, side_in, *refs):
    powers, refs = refs[:WIDTH], refs[WIDTH:]
    fields, (side, gram, acc) = (v0,) + refs[:WIDTH], refs[WIDTH:]
    planes = v0.shape[0]
    size = state[0, 0:1, 0:1]
    interior(fields, scale)
    gram[...] = basis_gram(powers, (), size, [(0, planes, LOW_PAIRS)], acc)


def inner_kernel(v0, state, early, *refs):
    powers, fields, (gram, acc) = refs[:WIDTH], (v0,) + refs[WIDTH : 2 * WIDTH], refs[2 * WIDTH :]
    inner = v0.shape[0] - 2 * WIDTH
    segments = [(WIDTH, inner, HIGH_PAIRS)]
    gram[...] = early[...] + basis_gram(powers, fields, state[0, 0:1, 0:1], segments, acc)


def fresh_wedge(use_a, where, got, scale, ghost_scale, state, early, v0, *refs):
    powers, refs = refs[:WIDTH], refs[WIDTH:]
    fields, gram = (v0,) + refs[WIDTH : 2 * WIDTH], refs[2 * WIDTH]
    ghosts, acc = refs[2 * WIDTH + 1 : -1], refs[-1]
    high, base, inward, keep = edge(where, use_a, v0.shape[0])
    wedge(fields, got, ghosts, scale, ghost_scale, base, inward, keep)
    if use_a:
        _, other, step, _ = edge(where, False, v0.shape[0])
        segments = [(lower(base, high), WIDTH, HIGH_PAIRS)] + side_segments(other, step, True)
    else:
        segments = side_segments(base, inward, False)
    value = early[...] + basis_gram(powers, fields, state[0, 0:1, 0:1], segments, acc)
    if use_a:
        gram[...] = value
    else:
        spread(gram, value)


def operator_columns(size, coef):
    powers = [unit(0)]
    for j in range(WIDTH - 1):
        image = (1.0 / size) * (powers[j] - unit(1 + j)) - CENTER * powers[j]
        powers.append((1.0 / HALF) * image if j == 0 else (2.0 / HALF) * image - powers[j - 1])
    rest = unit(WIDTH) - product(powers, coef)
    powers.append(rest / entry(coef, WIDTH))
    beyond = (HALF / 2) * (powers[WIDTH] + powers[WIDTH - 2]) + CENTER * powers[WIDTH - 1]
    beyond = powers[WIDTH - 1] - size * beyond
    out = [(1.0 / size) * (unit(0) - unit(1))]
    out += [chebyshev_column(1, k) for k in range(1, WIDTH - 1)]
    out.append(CENTER * unit(WIDTH - 1) + (HALF / 2) * (unit(WIDTH - 2) + beyond))
    return out + [chebyshev_column(WIDTH, k) for k in range(WIDTH, LAST)]


def finish_kernel(state, gram, *refs):
    count = LAST + 1
    refs, outs, rooms, sems = refs[:count], refs[count : count + 2], refs[count + 2 : count + 4], refs[-1]
    size = state[0]
    full = columns(gathered(gram), count)
    x, r, _ = steps(full, operator_columns(size, state[1]), LAST)
    back = to_powers(size, WIDTH - 1) + [unit(k) for k in range(WIDTH, count)]
    x, r = product(back, x), product(back, r)
    sx = [x[i : i + 1, :] for i in range(count)]
    sr = [r[i : i + 1, :] for i in range(count)]
    planes, ny, _ = refs[0].shape

    def body(z, carry):
        for row in range(0, ny, 8):
            tiles = [tile((ref, z), row) for ref in refs]
            ax, ar = sx[0] * tiles[0], sr[0] * tiles[0]
            for i in range(1, count):
                ar = ar + sr[i] * tiles[i]
                if i + 1 < count:
                    ax = ax + sx[i] * tiles[i]
            rooms[0][z, pl.ds(row, 8), :] = ax
            rooms[1][z, pl.ds(row, 8), :] = ar
        return carry

    copies = []
    part = planes // PARTS
    for k in range(PARTS):
        lax.fori_loop(k * part, (k + 1) * part, body, 0)
        here = pl.ds(k * part, part)
        for room, out in zip(rooms, outs):
            copies.append(pltpu.make_async_copy(room.at[here], out.at[here], sems.at[len(copies)]))
            copies[-1].start()
    for copy in copies:
        copy.wait()


def pairings(count):
    first = [(i, i ^ 1) for i in range(count) if i ^ 1 < count]
    second = [(i, i + 1) for i in range(1, count - 1, 2)]
    return first, second + [(j, i) for i, j in second]


def swap_a(side):
    return lax.ppermute(side, "slab", pairings(lax.axis_size("slab"))[0])


def swap_b(side):
    return lax.ppermute(side, "slab", pairings(lax.axis_size("slab"))[1])


def swap_all(value):
    return lax.all_to_all(value, "slab", 0, 0)


def local(right_side, diagonal):
    index = lax.axis_index("slab")
    count = lax.axis_size("slab")
    where = jnp.stack([index % 2, index > 0, index < count - 1]).astype(jnp.int32)
    field = right_side.shape
    some = lambda k: (k,) + field[1:]
    fields = [field] * WIDTH
    small = (ROWS, LANES)
    wide = (count,) + small
    ghosts = tuple(pltpu.VMEM(some(WIDTH - j), F32) for j in range(1, WIDTH))
    acc = lambda k: pltpu.VMEM((k, 8, LANES), F32)
    ghost_side = some(WIDTH - 1)

    message = some(2 * WIDTH - 1)
    rhs, diag = (pltpu.with_memory_space_constraint(a, pltpu.HBM) for a in (right_side, diagonal))
    semaphores = pltpu.SemaphoreType.DMA
    sa, sb = call(side_kernel, [message] * 2, scratch=(semaphores((4,)),), hbm=(1, 2))(where, rhs, diag)
    got_a = swap_a(sa)
    d, t0, *powers, sb, sampled = call(
        open_kernel,
        [field] * 2 + fields + [message, wide],
        {2: 2 + WIDTH},
        (acc(24), pltpu.VMEM(field, F32), semaphores((2,))),
        hbm=(0, 1),
    )(rhs, diag, sb)
    got_b = swap_b(sb)
    sampled = swap_all(sampled)
    inner = {6 + k: k for k in range(WIDTH)}
    side = some(WIDTH)
    *powers, gd_a, gd_b, v0, sa, sb, state = call(
        wedges_kernel, fields + [ghost_side] * 2 + [field, side, side, (2,) + small], inner, ghosts * 2
    )(where, got_a, got_b, d, sampled, t0, *powers)
    powers = [t0] + powers[:-1]
    got_a = swap_a(sa)
    *late, sb, early = call(fresh_kernel, fields + [side, small], {3: WIDTH}, (acc(56),))(v0, d, state, sb, *powers)
    got_b = swap_b(sb)
    early = call(inner_kernel, [small], scratch=(acc(56),))(v0, state, early, *powers, *late)[0]
    inner = {7 + WIDTH + k: k for k in range(WIDTH)}
    scratch = ghosts + (acc(56),)
    *late, early = call(functools.partial(fresh_wedge, True), fields + [small], inner, scratch)(
        where, got_a, d, gd_a, state, early, v0, *powers, *late
    )
    *late, gram = call(functools.partial(fresh_wedge, False), fields + [wide], inner, scratch)(
        where, got_b, d, gd_b, state, early, v0, *powers, *late
    )
    gram = swap_all(gram)
    rooms = (pltpu.VMEM(field, F32),) * 2 + (semaphores((2 * PARTS,)),)
    finish = call(finish_kernel, [field] * 2, scratch=rooms, out_space=pltpu.HBM)
    return tuple(finish(state, gram, *powers, v0, *late))


def solution(mesh):
    placed = (P("slab", "sys", None), P("slab", "sys", None))
    return jax.shard_map(
        local,
        mesh=mesh,
        in_specs=placed,
        out_specs=placed,
        check_vma=False,
    )
```
